8 devices in a mesh: dp: 2 (over z, y), tp: 4 (over x, core).
Axes of the slice: x: 2, y: 2, z: 1, core: 2. Of those that a mesh axis runs over, the one named last changes fastest.
Arguments:
- x_in: bfloat16 [2, 64, 3072], P('dp', 'tp'), parts along dimension 0
- start_pos: int32 [2], P('dp'), parts along dimension 0
- k_cache: bfloat16 [2, 4096, 8, 128], P('dp', None, 'tp'), parts along dimension 0
- v_cache: bfloat16 [2, 4096, 8, 128], P('dp', None, 'tp'), parts along dimension 0
- attn_gain: bfloat16 [3072], replicated
- w_query: bfloat16 [3072, 24, 128], P(None, 'tp')
- w_key: bfloat16 [3072, 8, 128], P(None, 'tp')
- w_value: bfloat16 [3072, 8, 128], P(None, 'tp')
- w_out: bfloat16 [24, 128, 3072], P('tp')
- mlp_gain: bfloat16 [3072], replicated
- w_gate: bfloat16 [3072, 8192], P(None, 'tp')
- w_up: bfloat16 [3072, 8192], P(None, 'tp')
- w_down: bfloat16 [8192, 3072], P('tp')
Outputs:
- output 1: bfloat16 [2, 64, 3072], P('dp', 'tp'), parts along dimension 0
- output 2: bfloat16 [2, 4096, 8, 128], P('dp', None, 'tp'), parts along dimension 0
- output 3: bfloat16 [2, 4096, 8, 128], P('dp', None, 'tp'), parts along dimension 0
There are 2 independent parts. The reference program is written for one: setup_inputs(seed, part) draws one part's arguments, and reference() takes and returns one part's arrays. A program takes and returns all parts, laid end to end along the dimension named above; an argument that names none is the same for every part.
All inputs are finite; a program needn't handle non-finite values.
Results may differ from the reference program's by a relative error of at most 0.0131868.
Values are sent between devices in bfloat16 or wider.
A program may use at most 1 GiB of HBM per device.

```python
import jax
import jax.numpy as jnp
from jax import lax

MODEL_DIM = 3072
Q_HEADS = 24
KV_HEADS = 8
HEAD_DIM = 128
FFN_DIM = 8192
WINDOW = 4096
BATCH_ROWS = 1
CHUNK_LEN = 64
ROPE_BASE = 10000.0
NORM_EPS = 1e-5
GROUP_SIZE = Q_HEADS // KV_HEADS
QUERY_BLOCK = min(CHUNK_LEN, 128)


def setup_inputs(seed: int = 0, part: int = 0) -> dict:
    part_keys = jax.random.split(jax.random.fold_in(jax.random.key(seed), part), 6)
    shared_keys = jax.random.split(jax.random.key(seed + 1), 9)
    cache_shape = (BATCH_ROWS, WINDOW, KV_HEADS, HEAD_DIM)
    x_in = jax.random.normal(part_keys[0], (BATCH_ROWS, CHUNK_LEN, MODEL_DIM), jnp.float32)
    row_starts = jax.random.randint(part_keys[1], (BATCH_ROWS,), 0, 3 * WINDOW)
    first_start = jax.random.randint(part_keys[2], (), WINDOW, 3 * WINDOW)
    start_pos = jnp.where(jnp.arange(BATCH_ROWS) == 0, first_start, row_starts)
    k_cache = 1.5 * jax.random.normal(part_keys[3], cache_shape, jnp.float32)
    v_mean = jax.random.normal(part_keys[4], (BATCH_ROWS, 1, KV_HEADS, HEAD_DIM), jnp.float32)
    v_cache = v_mean + jax.random.normal(part_keys[5], cache_shape, jnp.float32)
    attn_gain = 1.0 + 0.25 * jax.random.normal(shared_keys[0], (MODEL_DIM,), jnp.float32)
    w_query = (1.5 * MODEL_DIM ** -0.5) * jax.random.normal(shared_keys[1], (MODEL_DIM, Q_HEADS, HEAD_DIM), jnp.float32)
    w_key = (1.5 * MODEL_DIM ** -0.5) * jax.random.normal(shared_keys[2], (MODEL_DIM, KV_HEADS, HEAD_DIM), jnp.float32)
    w_value = MODEL_DIM ** -0.5 * jax.random.normal(shared_keys[3], (MODEL_DIM, KV_HEADS, HEAD_DIM), jnp.float32)
    w_out = (Q_HEADS * HEAD_DIM) ** -0.5 * jax.random.normal(shared_keys[4], (Q_HEADS, HEAD_DIM, MODEL_DIM), jnp.float32)
    mlp_gain = 1.0 + 0.25 * jax.random.normal(shared_keys[5], (MODEL_DIM,), jnp.float32)
    w_gate = MODEL_DIM ** -0.5 * jax.random.normal(shared_keys[6], (MODEL_DIM, FFN_DIM), jnp.float32)
    w_up = MODEL_DIM ** -0.5 * jax.random.normal(shared_keys[7], (MODEL_DIM, FFN_DIM), jnp.float32)
    w_down = FFN_DIM ** -0.5 * jax.random.normal(shared_keys[8], (FFN_DIM, MODEL_DIM), jnp.float32)
    return {
        'x_in': x_in.astype(jnp.bfloat16),
        'start_pos': start_pos.astype(jnp.int32),
        'k_cache': k_cache.astype(jnp.bfloat16),
        'v_cache': v_cache.astype(jnp.bfloat16),
        'attn_gain': attn_gain.astype(jnp.bfloat16),
        'w_query': w_query.astype(jnp.bfloat16),
        'w_key': w_key.astype(jnp.bfloat16),
        'w_value': w_value.astype(jnp.bfloat16),
        'w_out': w_out.astype(jnp.bfloat16),
        'mlp_gain': mlp_gain.astype(jnp.bfloat16),
        'w_gate': w_gate.astype(jnp.bfloat16),
        'w_up': w_up.astype(jnp.bfloat16),
        'w_down': w_down.astype(jnp.bfloat16),
    }


def rms_norm(rows, gain):
    rows32 = rows.astype(jnp.float32)
    inv_rms = lax.rsqrt(jnp.mean(rows32 * rows32, axis=-1, keepdims=True) + NORM_EPS)
    return (rows32 * inv_rms * gain.astype(jnp.float32)).astype(jnp.bfloat16)


def rotate(heads_in, positions):
    inv_freq = jnp.power(ROPE_BASE, -jnp.arange(0, HEAD_DIM, 2).astype(jnp.float32) / HEAD_DIM)
    angles = positions.astype(jnp.float32)[:, None] * inv_freq[None, :]
    cos_t = jnp.cos(angles)[:, None, :]
    sin_t = jnp.sin(angles)[:, None, :]
    pairs = heads_in.reshape(heads_in.shape[0], heads_in.shape[1], HEAD_DIM // 2, 2)
    even = pairs[..., 0]
    odd = pairs[..., 1]
    turned = jnp.stack([even * cos_t - odd * sin_t, even * sin_t + odd * cos_t], axis=-1)
    return turned.reshape(heads_in.shape)


def layer_row(x_row, start, k_old, v_old, attn_gain, w_query, w_key, w_value, w_out, mlp_gain, w_gate, w_up, w_down):
    positions = start + jnp.arange(CHUNK_LEN)
    normed = rms_norm(x_row, attn_gain)
    q_lin = jnp.dot(normed, w_query.reshape(MODEL_DIM, Q_HEADS * HEAD_DIM), preferred_element_type=jnp.float32)
    k_lin = jnp.dot(normed, w_key.reshape(MODEL_DIM, KV_HEADS * HEAD_DIM), preferred_element_type=jnp.float32)
    v_lin = jnp.dot(normed, w_value.reshape(MODEL_DIM, KV_HEADS * HEAD_DIM), preferred_element_type=jnp.float32)
    queries = rotate(q_lin.reshape(CHUNK_LEN, Q_HEADS, HEAD_DIM), positions).astype(jnp.bfloat16)
    k_chunk = rotate(k_lin.reshape(CHUNK_LEN, KV_HEADS, HEAD_DIM), positions).astype(jnp.bfloat16)
    v_chunk = v_lin.astype(jnp.bfloat16).reshape(CHUNK_LEN, KV_HEADS, HEAD_DIM)
    offsets = jnp.mod(jnp.arange(WINDOW) - start, WINDOW)
    cache_valid = (start - WINDOW + offsets) >= 0
    keys = jnp.concatenate([k_old, k_chunk], axis=0).astype(jnp.float32)
    values = jnp.concatenate([v_old, v_chunk], axis=0).astype(jnp.float32)
    n_blocks = CHUNK_LEN // QUERY_BLOCK
    q_tiles = queries.reshape(n_blocks, QUERY_BLOCK, KV_HEADS, GROUP_SIZE, HEAD_DIM)

    def attend_block(tile_pair):
        q_tile, block = tile_pair
        q_ids = block * QUERY_BLOCK + jnp.arange(QUERY_BLOCK)
        cache_mask = cache_valid[None, :] & (offsets[None, :] > q_ids[:, None])
        chunk_mask = jnp.arange(CHUNK_LEN)[None, :] <= q_ids[:, None]
        mask = jnp.concatenate([cache_mask, chunk_mask], axis=1)
        scores = jnp.einsum('qkge,ske->kgqs', q_tile.astype(jnp.float32), keys) * (HEAD_DIM ** -0.5)
        scores = jnp.where(mask[None, None], scores, -jnp.inf)
        attn_probs = jax.nn.softmax(scores, axis=-1).astype(jnp.bfloat16)
        mixed = jnp.einsum('kgqs,ske->qkge', attn_probs.astype(jnp.float32), values)
        return mixed.astype(jnp.bfloat16)

    mixed = lax.map(attend_block, (q_tiles, jnp.arange(n_blocks)))
    attn_out = jnp.dot(mixed.reshape(CHUNK_LEN, Q_HEADS * HEAD_DIM), w_out.reshape(Q_HEADS * HEAD_DIM, MODEL_DIM), preferred_element_type=jnp.float32)
    hidden = (x_row.astype(jnp.float32) + attn_out).astype(jnp.bfloat16)
    mlp_rows = rms_norm(hidden, mlp_gain)
    gate = jnp.dot(mlp_rows, w_gate, preferred_element_type=jnp.float32)
    up_proj = jnp.dot(mlp_rows, w_up, preferred_element_type=jnp.float32)
    activated = (jax.nn.silu(gate) * up_proj).astype(jnp.bfloat16)
    mlp_out = jnp.dot(activated, w_down, preferred_element_type=jnp.float32)
    x_out = (hidden.astype(jnp.float32) + mlp_out).astype(jnp.bfloat16)
    slots = jnp.mod(start + jnp.arange(CHUNK_LEN), WINDOW)
    k_new = k_old.at[slots].set(k_chunk)
    v_new = v_old.at[slots].set(v_chunk)
    return x_out, k_new, v_new


def reference(x_in, start_pos, k_cache, v_cache, attn_gain, w_query, w_key, w_value, w_out, mlp_gain, w_gate, w_up, w_down):
    def one_row(row_inputs):
        x_row, start, k_old, v_old = row_inputs
        return layer_row(x_row, start, k_old, v_old, attn_gain, w_query, w_key, w_value, w_out, mlp_gain, w_gate, w_up, w_down)

    x_out, k_new, v_new = lax.map(one_row, (x_in, start_pos, k_cache, v_cache))
    return x_out, k_new, v_new
```

```python
import functools

import jax
import jax.numpy as jnp
import numpy as np
from jax import lax
from jax.experimental import pallas as pl
from jax.experimental.pallas import tpu as pltpu
from jax.sharding import PartitionSpec as P

ROPE_BASE = 10000.0
NORM_EPS = 1e-5
MESH = pl.DeviceIdType.MESH
BF16 = jnp.bfloat16
F32 = jnp.float32
HD = 128
NCH = 4
KB = 512


def dot(a, b):
    return jnp.dot(a, b, preferred_element_type=F32)


def dot_t(a, b):
    return lax.dot_general(a, b, (((1,), (1,)), ((), ())), preferred_element_type=F32)


def layer_kernel(start_ref, invf_ref, x_hbm, g1_hbm, g2_hbm, kc_hbm, vc_hbm, wq_hbm, wk_hbm, wv_hbm, wo_hbm, wg_hbm, wu_hbm, wd_hbm,
                 xo_hbm, kn_hbm, vn_hbm,
                 xall, nbuf, g1, g2, kbuf, vbuf, wq, wk, wv, wo, wg, wu, wd,
                 sbuf, qbuf, kch, vch, obuf, part, rx1, cs, rx2, hbuf, ubuf, part2, rx4, cs2, rx5, xout, kout, vout,
                 ld_sem, st_sem, ag_send, ag_recv, s1, r1, s2, r2, s3, r3, s4, r4, s5, r5):
    T = xall.shape[0]
    D = xall.shape[1]
    CW = D // NCH
    HW = CW // 2
    tb = T // 4
    window = kbuf.shape[0] * 128
    me = lax.axis_index('tp')
    core = lax.rem(me, 2)
    chip = lax.div(me, 2)
    partner = chip * 2 + (1 - core)
    across = (1 - chip) * 2 + core

    def load(i, src, dst):
        return pltpu.make_async_copy(src, dst, ld_sem.at[i])

    def rows_of(owner):
        return pl.ds(pl.multiple_of(owner * tb, tb), tb)

    def remote(src, dst, send, recv, dev):
        return pltpu.make_async_remote_copy(src_ref=src, dst_ref=dst, send_sem=send, recv_sem=recv, device_id={'tp': dev}, device_id_type=MESH)

    barrier = pltpu.get_barrier_semaphore()
    for other in (partner, across):
        pl.semaphore_signal(barrier, inc=1, device_id={'tp': other}, device_id_type=MESH)

    own = xall.at[rows_of(me)]
    loads = [load(0, x_hbm, own), load(1, g1_hbm, g1), load(2, g2_hbm, g2), load(3, kc_hbm, kbuf), load(4, vc_hbm, vbuf),
             load(5, wk_hbm, wk), load(6, wv_hbm, wv), load(7, wq_hbm, wq), load(8, wo_hbm, wo), load(9, wg_hbm, wg),
             load(10, wu_hbm, wu), load(11, wd_hbm, wd)]
    for item in loads:
        item.start()
    pl.semaphore_wait(barrier, 2)

    loads[0].wait()
    to_partner = remote(own, own, ag_send.at[0], ag_recv.at[0], partner)
    to_across = remote(own, own, ag_send.at[1], ag_recv.at[1], across)
    to_across.start()
    to_partner.start()

    row = lax.broadcasted_iota(jnp.int32, (256, 256), 0)
    col = lax.broadcasted_iota(jnp.int32, (256, 256), 1)
    pick = jnp.where(col == 2 * lax.rem(row, 128) + lax.div(row, 128), 1.0, 0.0).astype(BF16)

    def split(a_ref, b_ref):
        def body(b, carry):
            both = jnp.concatenate([a_ref[b], b_ref[b]], axis=1)
            sep = dot(pick, both).astype(BF16)
            a_ref[b] = sep[:, :128]
            b_ref[b] = sep[:, 128:]
            return carry
        lax.fori_loop(0, a_ref.shape[0], body, 0, unroll=4)

    loads[3].wait()
    loads[4].wait()
    split(kbuf, vbuf)
    loads[5].wait()
    loads[6].wait()
    split(wk, wv)

    start = start_ref[0]
    lane = lax.broadcasted_iota(jnp.int32, (T, HD), 1)
    tok = lax.broadcasted_iota(jnp.int32, (T, HD), 0)
    angles = (start + tok).astype(F32) * invf_ref[...]
    cos_t = jnp.cos(angles)
    even = lax.rem(lane, 2) == 0
    sin_t = jnp.where(even, -jnp.sin(angles), jnp.sin(angles))

    def rope(h):
        swapped = jnp.where(even, pltpu.roll(h, HD - 1, 1), pltpu.roll(h, 1, 1))
        return h * cos_t + swapped * sin_t

    to_across.wait_recv()
    relay = xall.at[rows_of(across)]
    fwd = remote(relay, relay, ag_send.at[2], ag_recv.at[2], partner)
    fwd.start()
    to_partner.wait_recv()
    fwd.wait_recv()

    loads[1].wait()
    loads[2].wait()
    x32 = xall[...].astype(F32)
    inv = lax.rsqrt(jnp.mean(x32 * x32, axis=-1, keepdims=True) + NORM_EPS)
    nbuf[...] = (x32 * inv * g1[...].astype(F32)).astype(BF16)

    loads[7].wait()
    normed = nbuf[...]

    def split_rows(ref, g):
        return ref[:, g * 128:(g + 1) * 128, :].reshape(D, HD)

    k_lin = dot(normed, jnp.concatenate([split_rows(wk, 0), split_rows(wk, 1)], axis=1))
    v_lin = dot(normed, jnp.concatenate([split_rows(wv, 0), split_rows(wv, 1)], axis=1))
    kch[...] = jnp.zeros_like(kch)
    vch[...] = jnp.zeros_like(vch)
    for g in range(2):
        kch[g, :T] = rope(k_lin[:, g * HD:(g + 1) * HD]).astype(BF16)
        vch[g, :T] = v_lin[:, g * HD:(g + 1) * HD].astype(BF16)
    for pair in range(3):
        q_lin = dot(normed, jnp.concatenate([wq[2 * pair], wq[2 * pair + 1]], axis=1))
        for i in range(2):
            head = 2 * pair + i
            qbuf[head // 3, (head % 3) * T:(head % 3 + 1) * T] = rope(q_lin[:, i * HD:(i + 1) * HD]).astype(BF16)

    prow = lax.broadcasted_iota(jnp.int32, (2 * T, HD), 0)
    pcol = lax.broadcasted_iota(jnp.int32, (2 * T, HD), 1)
    for src, dst in ((kch, kout), (vch, vout)):
        mix = sum(dot(jnp.where(prow == 2 * pcol + g, 1.0, 0.0).astype(BF16), src[g]) for g in range(2))
        dst[...] = mix.astype(BF16)
    store_k = pltpu.make_async_copy(kout, kn_hbm, st_sem.at[0])
    store_v = pltpu.make_async_copy(vout, vn_hbm, st_sem.at[1])
    store_k.start()
    store_v.start()

    R = 3 * T
    coef = HD ** -0.5 * float(np.log2(np.e))
    q_tok = lax.rem(lax.broadcasted_iota(jnp.int32, (R, 1), 0), T)
    cl = lax.broadcasted_iota(jnp.int32, (R, HD), 1)
    lanes_kb = lax.broadcasted_iota(jnp.int32, (1, KB), 1)
    nb = KB // 128
    for g in range(2):
        q_g = qbuf[g]
        s_c = dot_t(q_g, kch[g])
        s_c = jnp.where(cl <= q_tok, s_c, -jnp.inf)

        def score(i, top):
            keys = kbuf[pl.ds(i * nb, nb), g * 128:(g + 1) * 128, :].reshape(KB, HD)
            s = dot_t(q_g, keys)
            off = lax.rem(lanes_kb + i * KB - start + 4 * window, window)
            off = jnp.where(start - window + off >= 0, off, -1)
            s = jnp.where(off > q_tok, s, -jnp.inf)
            sbuf[i] = s
            for j in range(nb):
                top = jnp.maximum(top, s[:, j * 128:(j + 1) * 128])
            return top

        top = lax.fori_loop(0, window // KB, score, s_c)
        top = jnp.max(top, axis=1, keepdims=True)
        e_c = jnp.exp2((s_c - top) * coef)

        def expo(i, mass):
            e = jnp.exp2((sbuf[i] - top) * coef)
            sbuf[i] = e
            for j in range(nb):
                mass = mass + e[:, j * 128:(j + 1) * 128]
            return mass

        mass = lax.fori_loop(0, window // KB, expo, e_c)
        scale = 1.0 / jnp.sum(mass, axis=1, keepdims=True)

        def weigh(i, acc):
            vals = vbuf[pl.ds(i * nb, nb), g * 128:(g + 1) * 128, :].reshape(KB, HD)
            return acc + dot((sbuf[i] * scale).astype(BF16), vals)

        acc = dot((e_c * scale).astype(BF16), vch[g])
        acc = lax.fori_loop(0, window // KB, weigh, acc)
        for j in range(3):
            head = 3 * g + j
            obuf[:, head * HD:(head + 1) * HD] = acc[j * T:(j + 1) * T].astype(BF16)

    loads[8].wait()
    mixed = obuf[...]
    sends = []
    for c in range(NCH):
        p = dot(mixed, wo[:, c * CW:(c + 1) * CW]).astype(BF16)
        part[c, 0] = p[:, :HW]
        part[c, 1] = p[:, HW:]
        cp = remote(part.at[c, 1 - core], rx1.at[c], s1.at[c], r1.at[c], partner)
        cp.start()
        sends.append(cp)
    hop2 = []
    for c in range(NCH):
        sends[c].wait_recv()
        cs[c] = (part[c, core].astype(F32) + rx1[c].astype(F32)).astype(BF16)
        cp = remote(cs.at[c], rx2.at[c], s2.at[c], r2.at[c], across)
        cp.start()
        hop2.append(cp)
    hop3 = []
    for c in range(NCH):
        hop2[c].wait_recv()
        cols = pl.ds(pl.multiple_of(c * CW + core * HW, 128), HW)
        total = cs[c].astype(F32) + rx2[c].astype(F32)
        hbuf[c, core] = (xall[:, cols].astype(F32) + total).astype(BF16)
        cp = remote(hbuf.at[c, core], hbuf.at[c, core], s3.at[c], r3.at[c], partner)
        cp.start()
        hop3.append(cp)
    sq = jnp.zeros((T, 1), F32)
    for c in range(NCH):
        hop3[c].wait_recv()
        for i in range(2):
            h32 = hbuf[c, i].astype(F32)
            sq = sq + jnp.sum(h32 * h32, axis=-1, keepdims=True)
    inv = lax.rsqrt(sq / D + NORM_EPS)
    for c in range(NCH):
        for i in range(2):
            lo = c * CW + i * HW
            nbuf[:, lo:lo + HW] = (hbuf[c, i].astype(F32) * inv * g2[:, lo:lo + HW].astype(F32)).astype(BF16)

    loads[9].wait()
    loads[10].wait()
    FB = 512
    F = wg.shape[1]

    def gate_up(j, carry):
        cols = pl.ds(pl.multiple_of(j * FB, FB), FB)
        m = nbuf[...]
        gate = dot(m, wg[:, cols])
        up = dot(m, wu[:, cols])
        ubuf[:, cols] = (gate * jax.nn.sigmoid(gate) * up).astype(BF16)
        return carry

    lax.fori_loop(0, F // FB, gate_up, 0)
    loads[11].wait()
    act = ubuf[...]
    hop4 = []
    for c in range(NCH):
        p = dot(act, wd[:, c * CW:(c + 1) * CW]).astype(BF16)
        for o in range(4):
            part2[c, o % 2, (o // 2) * tb:(o // 2 + 1) * tb] = p[o * tb:(o + 1) * tb]
        cp = remote(part2.at[c, 1 - core], rx4.at[c], s4.at[c], r4.at[c], partner)
        cp.start()
        hop4.append(cp)
    hop5 = []
    mine = rows_of(chip)
    theirs = rows_of(1 - chip)
    for c in range(NCH):
        hop4[c].wait_recv()
        cs2[c] = (part2[c, core, theirs].astype(F32) + rx4[c, theirs].astype(F32)).astype(BF16)
        cp = remote(cs2.at[c], rx5.at[c], s5.at[c], r5.at[c], across)
        cp.start()
        hop5.append(cp)
    outs = []
    for c in range(NCH):
        hop5[c].wait_recv()
        local = part2[c, core, mine].astype(F32) + rx4[c, mine].astype(F32) + rx5[c].astype(F32)
        for i in range(2):
            lo = c * CW + i * HW
            xout[:, lo:lo + HW] = (hbuf[c, i, rows_of(me)].astype(F32) + local[:, i * HW:(i + 1) * HW]).astype(BF16)
    store_x = pltpu.make_async_copy(xout, xo_hbm, st_sem.at[2])
    store_x.start()
    for cp in [to_partner, to_across, fwd] + sends + hop2 + hop3 + hop4 + hop5:
        cp.wait_send()
    store_k.wait()
    store_v.wait()
    store_x.wait()


def cache_kernel(start_ref, kc, vc, kch, vch, xin, kn, vn, xo, kbuf, vbuf, kcb, vcb, xb, in_sem, out_sem):
    nblk = kc.shape[0]
    per = kc.shape[1]
    rows = nblk * per
    small = [pltpu.make_async_copy(kch, kcb, in_sem.at[0, nblk]), pltpu.make_async_copy(vch, vcb, in_sem.at[1, nblk]),
             pltpu.make_async_copy(xin, xb, in_sem.at[2, nblk])]
    for cp in small:
        cp.start()
    reads = []
    for b in range(nblk):
        for i, (src, dst) in enumerate(((kc, kbuf), (vc, vbuf))):
            cp = pltpu.make_async_copy(src.at[b], dst.at[b], in_sem.at[i, b])
            cp.start()
            reads.append(cp)
    start = start_ref[0]
    for cp in small:
        cp.wait()
    xw = pltpu.make_async_copy(xb, xo, out_sem.at[2, 0])
    xw.start()
    first = lax.rem(2 * start, rows)
    writes = [xw]
    jrow = lax.broadcasted_iota(jnp.int32, (per, 128), 0)
    jcol = lax.broadcasted_iota(jnp.int32, (per, 128), 1)
    for b in range(nblk):
        for i in range(2):
            reads[2 * b + i].wait()
        lo = b * per
        ahead = lax.rem(lo - first + rows, rows)
        touched = (ahead < 128) | (ahead > rows - per)

        @pl.when(touched)
        def _():
            rel = lax.rem(jrow + lo - first + rows, rows)
            hot = jnp.where(rel == jcol, 1.0, 0.0).astype(BF16)
            inside = rel < 128
            kbuf[b] = jnp.where(inside, dot(hot, kcb[...]), kbuf[b].astype(F32)).astype(BF16)
            vbuf[b] = jnp.where(inside, dot(hot, vcb[...]), vbuf[b].astype(F32)).astype(BF16)

        for i, (src, dst) in enumerate(((kbuf, kn), (vbuf, vn))):
            cp = pltpu.make_async_copy(src.at[b], dst.at[b], out_sem.at[i, b])
            cp.start()
            writes.append(cp)
    for cp in writes:
        cp.wait()


def solution(mesh):
    row_spec = P('dp', 'tp', None)
    cache_spec = P('dp', None, 'tp', None)
    head_cols = P(None, 'tp', None)
    in_specs = (row_spec, P('dp'), cache_spec, cache_spec, P(), head_cols, head_cols, head_cols, P('tp', None, None), P(), P(None, 'tp'), P(None, 'tp'), P('tp', None))
    out_specs = (row_spec, cache_spec, cache_spec)

    def local_layer(x_in, start_pos, k_cache, v_cache, attn_gain, w_query, w_key, w_value, w_out, mlp_gain, w_gate, w_up, w_down):
        _, tb, D = x_in.shape
        T = 4 * tb
        window = k_cache.shape[1]
        F = w_gate.shape[1]
        CW = D // NCH
        HW = CW // 2
        qh = w_query.shape[1]
        invf = jnp.asarray(np.repeat(ROPE_BASE ** (-np.arange(0, HD, 2) / HD), 2).astype(np.float32)[None])
        blocks = window // 128
        kc = k_cache.reshape(blocks, 256, HD)
        vc = v_cache.reshape(blocks, 256, HD)
        wk = w_key.reshape(D // 128, 256, HD)
        wv = w_value.reshape(D // 128, 256, HD)
        any_spec = pl.BlockSpec(memory_space=pl.ANY)
        vmem = pltpu.VMEM
        dma = pltpu.SemaphoreType.DMA
        x_out, k_ch, v_ch = pl.pallas_call(
            layer_kernel,
            name='layer',
            out_shape=(jax.ShapeDtypeStruct((tb, D), BF16), jax.ShapeDtypeStruct((2 * T, HD), BF16), jax.ShapeDtypeStruct((2 * T, HD), BF16)),
            in_specs=[pl.BlockSpec(memory_space=pltpu.SMEM), pl.BlockSpec(memory_space=pltpu.VMEM)] + [any_spec] * 12,
            out_specs=(any_spec,) * 3,
            scratch_shapes=[
                vmem((T, D), BF16), vmem((T, D), BF16), vmem((1, D), BF16), vmem((1, D), BF16),
                vmem((blocks, 256, HD), BF16), vmem((blocks, 256, HD), BF16),
                vmem((qh, D, HD), BF16), vmem((D // 128, 256, HD), BF16), vmem((D // 128, 256, HD), BF16),
                vmem((qh * HD, D), BF16), vmem((D, F), BF16), vmem((D, F), BF16), vmem((F, D), BF16),
                vmem((window // KB, 3 * T, KB), F32), vmem((2, 3 * T, HD), BF16), vmem((2, 128, HD), BF16), vmem((2, 128, HD), BF16),
                vmem((T, qh * HD), BF16),
                vmem((NCH, 2, T, HW), BF16), vmem((NCH, T, HW), BF16), vmem((NCH, T, HW), BF16), vmem((NCH, T, HW), BF16),
                vmem((NCH, 2, T, HW), BF16), vmem((T, F), BF16),
                vmem((NCH, 2, 2 * tb, CW), BF16), vmem((NCH, 2 * tb, CW), BF16), vmem((NCH, tb, CW), BF16), vmem((NCH, tb, CW), BF16),
                vmem((tb, D), BF16), vmem((2 * T, HD), BF16), vmem((2 * T, HD), BF16),
                dma((12,)), dma((3,)), dma((3,)), dma((3,)),
            ] + [dma((NCH,))] * 10,
            compiler_params=pltpu.CompilerParams(collective_id=0, has_side_effects=True, vmem_limit_bytes=67043328),
        )(start_pos, invf, x_in.reshape(tb, D), attn_gain.reshape(1, D), mlp_gain.reshape(1, D), kc, vc, w_query.transpose(1, 0, 2), wk, wv,
          w_out.reshape(qh * HD, D), w_gate, w_up, w_down)
        nblk = 8
        per = 2 * window // nblk
        k_new, v_new, x_fin = pl.pallas_call(
            cache_kernel,
            name='cache',
            out_shape=(jax.ShapeDtypeStruct((nblk, per, HD), BF16),) * 2 + (jax.ShapeDtypeStruct((tb, D), BF16),),
            in_specs=[pl.BlockSpec(memory_space=pltpu.SMEM)] + [any_spec] * 5,
            out_specs=(any_spec,) * 3,
            scratch_shapes=[vmem((nblk, per, HD), BF16)] * 2 + [vmem((2 * T, HD), BF16)] * 2 + [vmem((tb, D), BF16), dma((3, nblk + 1)), dma((3, nblk))],
        )(start_pos, k_cache.reshape(nblk, per, HD), v_cache.reshape(nblk, per, HD), k_ch, v_ch, x_out)
        return x_fin.reshape(x_in.shape), k_new.reshape(k_cache.shape), v_new.reshape(v_cache.shape)

    return jax.shard_map(local_layer, mesh=mesh, in_specs=in_specs, out_specs=out_specs, check_vma=False)
```

```python
import functools

import jax
import jax.numpy as jnp
import numpy as np
from jax import lax
from jax.experimental import pallas as pl
from jax.experimental.pallas import tpu as pltpu
from jax.sharding import PartitionSpec as P

ROPE_BASE = 10000.0
NORM_EPS = 1e-5
MESH = pl.DeviceIdType.MESH
BF16 = jnp.bfloat16
F32 = jnp.float32
HD = 128
NCH = 6
NCH2 = 6
NAG = 4
LAG = 4
KB = 512


def dot(a, b):
    return jnp.dot(a, b, preferred_element_type=F32)


def dot_t(a, b):
    return lax.dot_general(a, b, (((1,), (1,)), ((), ())), preferred_element_type=F32)


class Phases:
    def __init__(self):
        self.scope = None

    def __call__(self, name):
        self.close()
        self.scope = jax.named_scope(name)
        self.scope.__enter__()

    def close(self):
        if self.scope is not None:
            self.scope.__exit__(None, None, None)
        self.scope = None


def layer_kernel(start_hbm, invf_hbm, x_hbm, g1_hbm, g2_hbm, kc_hbm, vc_hbm, wq_hbm, wk_hbm, wv_hbm, wo_hbm, wg_hbm, wu_hbm, wd_hbm,
                 xo_hbm, kn_hbm, vn_hbm,
                 start_s, invf, xown, xh, nbuf, g1, g2, kbuf, vbuf, wq, wk, wv, wo, wg, wu, wd,
                 qacc, offb, sbuf, qbuf, kch, vch, obuf, part, rx1, cs, rx2, hbuf, gacc, ubuf, part2, rx4, cs2, rx5, xout, kout, vout,
                 ld_sem, st_sem, agp_s, agp_r, aga_s, aga_r, agf_s, agf_r, xs_s, xs_r, s1, r1, s2, r2, s3, r3, s4, r4, s5, r5):
    phase = Phases()
    phase('entry')
    T, D = nbuf.shape
    half = D // 2
    HW = half // NCH
    CW = D // NCH2
    AW = D // NAG
    tb = T // 4
    window = kbuf.shape[0] * 128
    F = wg.shape[1]
    me = lax.axis_index('tp')
    core = lax.rem(me, 2)
    chip = lax.div(me, 2)
    partner = chip * 2 + (1 - core)
    across = (1 - chip) * 2 + core
    diag = (1 - chip) * 2 + (1 - core)

    def load(i, src, dst):
        return pltpu.make_async_copy(src, dst, ld_sem.at[i])

    def rows_of(owner):
        return pl.ds(pl.multiple_of(owner * tb, tb), tb)

    def half_of(which):
        return pl.ds(pl.multiple_of(which * half, 128), half)

    def remote(src, dst, send, recv, dev):
        return pltpu.make_async_remote_copy(src_ref=src, dst_ref=dst, send_sem=send, recv_sem=recv, device_id={'tp': dev}, device_id_type=MESH)

    def wide(gain, lo, n):
        return jnp.concatenate([gain[i:i + 1] for i in range(lo // HD, (lo + n) // HD)], axis=1)

    barrier = pltpu.get_barrier_semaphore()
    for other in (across, diag, partner):
        pl.semaphore_signal(barrier, inc=1, device_id={'tp': other}, device_id_type=MESH)

    own = rows_of(me)
    loads = [load(0, x_hbm, xown), load(1, g1_hbm, g1), load(2, g2_hbm, g2), load(12, start_hbm, start_s), load(13, invf_hbm, invf),
             load(14, x_hbm.at[:, half_of(core)], xh.at[own]),
             load(3, kc_hbm, kbuf), load(4, vc_hbm, vbuf),
             load(5, wk_hbm, wk), load(6, wv_hbm, wv), load(7, wq_hbm, wq), load(8, wo_hbm, wo), load(9, wg_hbm, wg),
             load(10, wu_hbm, wu), load(11, wd_hbm, wd)]
    (ld_x, ld_g1, ld_g2, ld_start, ld_invf, ld_xh, ld_kc, ld_vc, ld_wk, ld_wv, ld_wq, ld_wo, ld_wg, ld_wu, ld_wd) = loads
    for item in loads:
        item.start()

    ld_x.wait()
    ld_g1.wait()
    x32 = xown[...].astype(F32)
    inv = lax.rsqrt(jnp.mean(x32 * x32, axis=-1, keepdims=True) + NORM_EPS)
    nbuf[own] = (x32 * inv * wide(g1[...].astype(F32), 0, D)).astype(BF16)
    pl.semaphore_wait(barrier, 3)
    ag_a = []
    for c in range(NAG):
        piece = nbuf.at[own, pl.ds(c * AW, AW)]
        ag_a.append(remote(piece, piece, aga_s.at[c], aga_r.at[c], across))
        ag_a[c].start()
    ag_p = remote(nbuf.at[own], nbuf.at[own], agp_s.at[0], agp_r.at[0], partner)
    ag_p.start()

    row = lax.broadcasted_iota(jnp.int32, (256, 256), 0)
    col = lax.broadcasted_iota(jnp.int32, (256, 256), 1)
    pick = jnp.where(col == 2 * lax.rem(row, 128) + lax.div(row, 128), 1.0, 0.0).astype(BF16)

    def split(a_ref, b_ref, lo, hi):
        def body(b, carry):
            both = jnp.concatenate([a_ref[b], b_ref[b]], axis=1)
            sep = dot(pick, both).astype(BF16)
            a_ref[b] = sep[:, :128]
            b_ref[b] = sep[:, 128:]
            return carry
        lax.fori_loop(lo, hi, body, 0, unroll=min(8, hi - lo))

    phase('wait_cache')
    ld_kc.wait()
    ld_vc.wait()
    phase('split_cache')
    split(kbuf, vbuf, 0, kbuf.shape[0])
    phase('wait_wkv')
    ld_wk.wait()
    ld_wv.wait()
    ag_f = []
    per_ag = wk.shape[0] // NAG
    for c in range(NAG):
        phase(f'wait_across{c}')
        ag_a[c].wait_recv()
        piece = nbuf.at[rows_of(across), pl.ds(c * AW, AW)]
        ag_f.append(remote(piece, piece, agf_s.at[c], agf_r.at[c], partner))
        ag_f[c].start()
        phase(f'split_wkv{c}')
        split(wk, wv, c * per_ag, (c + 1) * per_ag)

    x_sends = [remote(xown.at[:, half_of(core)], xh.at[own], xs_s.at[0], xs_r.at[0], across),
               remote(xown.at[:, half_of(1 - core)], xh.at[own], xs_s.at[1], xs_r.at[1], diag),
               remote(xown.at[:, half_of(1 - core)], xh.at[own], xs_s.at[2], xs_r.at[2], partner)]
    for cp in x_sends:
        cp.start()

    phase('trig')
    ld_start.wait()
    ld_invf.wait()
    start = start_s[0]
    lane = lax.broadcasted_iota(jnp.int32, (T, HD), 1)
    tok = lax.broadcasted_iota(jnp.int32, (T, HD), 0)
    angles = (start + tok).astype(F32) * invf[...]
    cos_t = jnp.cos(angles)
    even = lax.rem(lane, 2) == 0
    sin_t = jnp.sin(angles)
    sin_t = jnp.where(even, -sin_t, sin_t)
    slot = lax.broadcasted_iota(jnp.int32, (8, window), 1)
    off = lax.rem(slot - start + 4 * window, window)
    offb[...] = jnp.where(start - window + off >= 0, off, -1)

    def rope(h):
        swapped = jnp.where(even, pltpu.roll(h, HD - 1, 1), pltpu.roll(h, 1, 1))
        return h * cos_t + swapped * sin_t

    def split_rows(ref, g, c):
        return ref[c * per_ag:(c + 1) * per_ag, g * 128:(g + 1) * 128, :].reshape(AW, HD)

    ag_p.wait_recv()
    ld_wq.wait()
    kch[...] = jnp.zeros_like(kch)
    vch[...] = jnp.zeros_like(vch)
    for c in range(NAG):
        phase(f'wait_fwd{c}')
        ag_f[c].wait_recv()
        phase(f'qkv{c}')
        rows = nbuf[:, c * AW:(c + 1) * AW]
        for o in range(5):
            if o < 3:
                w = jnp.concatenate([wq[2 * o, c * AW:(c + 1) * AW], wq[2 * o + 1, c * AW:(c + 1) * AW]], axis=1)
            else:
                ref = wk if o == 3 else wv
                w = jnp.concatenate([split_rows(ref, 0, c), split_rows(ref, 1, c)], axis=1)
            p = dot(rows, w)
            qacc[o] = p if c == 0 else qacc[o] + p
    phase('rope')
    for g in range(2):
        kch[g, :T] = rope(qacc[3, :, g * HD:(g + 1) * HD]).astype(BF16)
        vch[g, :T] = qacc[4, :, g * HD:(g + 1) * HD].astype(BF16)
    for head in range(6):
        qbuf[head // 3, (head % 3) * T:(head % 3 + 1) * T] = rope(qacc[head // 2, :, (head % 2) * HD:(head % 2 + 1) * HD]).astype(BF16)

    phase('kvout')
    prow = lax.broadcasted_iota(jnp.int32, (2 * T, HD), 0)
    pcol = lax.broadcasted_iota(jnp.int32, (2 * T, HD), 1)
    for src, dst in ((kch, kout), (vch, vout)):
        mix = sum(dot(jnp.where(prow == 2 * pcol + g, 1.0, 0.0).astype(BF16), src[g]) for g in range(2))
        dst[...] = mix.astype(BF16)
    store_k = pltpu.make_async_copy(kout, kn_hbm, st_sem.at[0])
    store_v = pltpu.make_async_copy(vout, vn_hbm, st_sem.at[1])
    store_k.start()
    store_v.start()

    phase('attn')
    coef = HD ** -0.5 * float(np.log2(np.e))
    nblk = window // KB
    nb = KB // 128
    q_tok = lax.broadcasted_iota(jnp.int32, (T, HD), 0)
    q_tok3 = q_tok.reshape(T // 8, 8, HD)
    k_idx = lax.broadcasted_iota(jnp.int32, (T, HD), 1)

    def blocks(ref, g, i):
        return ref[i * nb:(i + 1) * nb, g * 128:(g + 1) * 128, :].reshape(KB, HD)

    top, mass, s_c = [[None] * 3, [None] * 3], [[None] * 3, [None] * 3], [[None] * 3, [None] * 3]
    peak, e_c, scale, acc = [[None] * 3, [None] * 3], [[None] * 3, [None] * 3], [[None] * 3, [None] * 3], [None, None]

    def score_chunk(g):
        s = dot_t(qbuf[g], kch[g])
        for h in range(3):
            s_c[g][h] = jnp.where(k_idx <= q_tok, s[h * T:(h + 1) * T], -jnp.inf)
            top[g][h] = s_c[g][h]

    def score(g, i):
        s = dot_t(qbuf[g], blocks(kbuf, g, i))
        for j in range(nb):
            o = offb[:, i * KB + j * 128:i * KB + (j + 1) * 128][None]
            keep = o > q_tok3
            for h in range(3):
                piece = s[h * T:(h + 1) * T, j * 128:(j + 1) * 128].reshape(T // 8, 8, HD)
                piece = jnp.where(keep, piece, -jnp.inf).reshape(T, HD)
                sbuf[g, i, h * T:(h + 1) * T, j * 128:(j + 1) * 128] = piece
                top[g][h] = jnp.maximum(top[g][h], piece)

    def expo_chunk(g):
        for h in range(3):
            peak[g][h] = jnp.max(top[g][h], axis=1, keepdims=True)
            e_c[g][h] = jnp.exp2((s_c[g][h] - peak[g][h]) * coef)
            mass[g][h] = e_c[g][h]

    def expo(g, h, i):
        e = jnp.exp2((sbuf[g, i, h * T:(h + 1) * T] - peak[g][h]) * coef)
        sbuf[g, i, h * T:(h + 1) * T] = e
        for j in range(nb):
            mass[g][h] = mass[g][h] + e[:, j * 128:(j + 1) * 128]

    def weigh_chunk(g):
        for h in range(3):
            scale[g][h] = 1.0 / jnp.sum(mass[g][h], axis=1, keepdims=True)
        p = jnp.concatenate([(e_c[g][h] * scale[g][h]).astype(BF16) for h in range(3)], axis=0)
        acc[g] = dot(p, vch[g])

    def weigh(g, i):
        p = jnp.concatenate([(sbuf[g, i, h * T:(h + 1) * T] * scale[g][h]).astype(BF16) for h in range(3)], axis=0)
        acc[g] = acc[g] + dot(p, blocks(vbuf, g, i))

    order = [(h, i) for h in range(3) for i in range(nblk)]
    score_chunk(0)
    for i in range(nblk):
        score(0, i)
    score_chunk(1)
    expo_chunk(0)
    for i in range(nblk):
        score(1, i)
        for h, k in order[3 * i:3 * i + 3]:
            expo(0, h, k)
    expo_chunk(1)
    weigh_chunk(0)
    for i in range(nblk):
        weigh(0, i)
        for h, k in order[3 * i:3 * i + 3]:
            expo(1, h, k)
    weigh_chunk(1)
    for i in range(nblk):
        weigh(1, i)
    for g in range(2):
        for h in range(3):
            head = 3 * g + h
            obuf[:, head * HD:(head + 1) * HD] = acc[g][h * T:(h + 1) * T].astype(BF16)

    phase('oproj')
    ld_wo.wait()
    hop1, hop2, hop3, hop4, hop5 = [], [], [], [], []
    for c in range(NCH):
        for i in range(2):
            lo = i * half + c * HW
            part[c, i] = dot(obuf[...], wo[:, lo:lo + HW]).astype(BF16)
        hop1.append(remote(part.at[c, 1 - core], rx1.at[c], s1.at[c], r1.at[c], partner))
        hop1[c].start()
    phase('hop1')
    for c in range(NCH):
        hop1[c].wait_recv()
        cs[c] = (part[c, core].astype(F32) + rx1[c].astype(F32)).astype(BF16)
        hop2.append(remote(cs.at[c], rx2.at[c], s2.at[c], r2.at[c], across))
        hop2[c].start()

    phase('hop2')
    for cp in x_sends:
        cp.wait_recv()
    ld_xh.wait()
    ld_g2.wait()
    gain2 = g2[...].astype(F32)
    g_top = jnp.maximum(jnp.max(jnp.max(jnp.abs(gain2), axis=1, keepdims=True), axis=0, keepdims=True), 1e-30)
    gain2 = gain2 / g_top
    ld_wg.wait()
    ld_wu.wait()
    squares = []

    def gate_up(c):
        hop3[c].wait_recv()
        phase(f'gateup{c}')
        lhs = []
        for i in range(2):
            h32 = hbuf[c, i].astype(F32)
            lhs.append((h32 * wide(gain2, i * half + c * HW, HW)).astype(BF16))
            for j in range(HW // 128):
                piece = h32[:, j * 128:(j + 1) * 128]
                squares.append(piece * piece if not squares else squares.pop() + piece * piece)
        for k, w in enumerate((wg, wu)):
            for lo in range(0, F, 512):
                p = sum(dot(lhs[i], w[i * half + c * HW:i * half + (c + 1) * HW, lo:lo + 512]) for i in range(2))
                gacc[k, :, lo:lo + 512] = p if c == 0 else gacc[k, :, lo:lo + 512] + p

    for c in range(NCH):
        phase(f'hop2_{c}')
        hop2[c].wait_recv()
        total = cs[c].astype(F32) + rx2[c].astype(F32)
        hbuf[c, core] = (xh[:, c * HW:(c + 1) * HW].astype(F32) + total).astype(BF16)
        hop3.append(remote(hbuf.at[c, core], hbuf.at[c, core], s3.at[c], r3.at[c], partner))
        hop3[c].start()
        if c >= 2:
            gate_up(c - 2)
    for c in range(NCH - 2, NCH):
        phase(f'hop3_{c}')
        gate_up(c)
    phase('act')
    inv2 = lax.rsqrt(jnp.sum(squares[0], axis=-1, keepdims=True) / D + NORM_EPS)
    inv2 = inv2 * g_top
    gate = jnp.where(inv2 > 0, gacc[0] * inv2, 0.0)
    up = jnp.where(inv2 > 0, gacc[1] * inv2, 0.0)
    ubuf[...] = (gate * jax.nn.sigmoid(gate) * up).astype(BF16)

    phase('down')
    ld_wd.wait()
    mine = rows_of(chip)
    theirs = rows_of(1 - chip)

    def chip_sum(c):
        hop4[c].wait_recv()
        cs2[c] = (part2[c, core, theirs].astype(F32) + rx4[c, theirs].astype(F32)).astype(BF16)
        hop5.append(remote(cs2.at[c], rx5.at[c], s5.at[c], r5.at[c], across))
        hop5[c].start()

    for c in range(NCH2):
        p = dot(ubuf[...], wd[:, c * CW:(c + 1) * CW]).astype(BF16)
        for o in range(4):
            part2[c, o % 2, (o // 2) * tb:(o // 2 + 1) * tb] = p[o * tb:(o + 1) * tb]
        hop4.append(remote(part2.at[c, 1 - core], rx4.at[c], s4.at[c], r4.at[c], partner))
        hop4[c].start()
        if c >= LAG:
            chip_sum(c - LAG)
    phase('hop4')
    for c in range(NCH2 - LAG, NCH2):
        chip_sum(c)
    phase('hop5')
    for c in range(NCH2):
        hop5[c].wait_recv()
        local = part2[c, core, mine].astype(F32) + rx4[c, mine].astype(F32) + rx5[c].astype(F32)
        for j in range(CW // HW):
            lo = c * CW + j * HW
            h_own = hbuf[(lo % half) // HW, lo // half, own].astype(F32)
            xout[:, lo:lo + HW] = (h_own + local[:, j * HW:(j + 1) * HW]).astype(BF16)
    store_x = pltpu.make_async_copy(xout, xo_hbm, st_sem.at[2])
    phase('fin')
    store_x.start()
    for cp in ag_a + [ag_p] + ag_f + x_sends + hop1 + hop2 + hop3 + hop4 + hop5:
        cp.wait_send()
    store_k.wait()
    store_v.wait()
    store_x.wait()
    phase.close()


def cache_kernel(start_ref, kc, vc, kch, vch, xin, kn, vn, xo, kbuf, vbuf, kcb, vcb, xb, in_sem, out_sem):
    nblk = kc.shape[0]
    per = kc.shape[1]
    rows = nblk * per
    small = [pltpu.make_async_copy(kch, kcb, in_sem.at[0, nblk]), pltpu.make_async_copy(vch, vcb, in_sem.at[1, nblk]),
             pltpu.make_async_copy(xin, xb, in_sem.at[2, nblk])]
    for cp in small:
        cp.start()
    reads = []
    for b in range(nblk):
        for i, (src, dst) in enumerate(((kc, kbuf), (vc, vbuf))):
            cp = pltpu.make_async_copy(src.at[b], dst.at[b], in_sem.at[i, b])
            cp.start()
            reads.append(cp)
    start = start_ref[0]
    for cp in small:
        cp.wait()
    xw = pltpu.make_async_copy(xb, xo, out_sem.at[2, 0])
    xw.start()
    first = lax.rem(2 * start, rows)
    writes = [xw]
    jrow = lax.broadcasted_iota(jnp.int32, (per, 128), 0)
    jcol = lax.broadcasted_iota(jnp.int32, (per, 128), 1)
    for b in range(nblk):
        for i in range(2):
            reads[2 * b + i].wait()
        lo = b * per
        ahead = lax.rem(lo - first + rows, rows)
        touched = (ahead < 128) | (ahead > rows - per)

        @pl.when(touched)
        def _():
            rel = lax.rem(jrow + lo - first + rows, rows)
            hot = jnp.where(rel == jcol, 1.0, 0.0).astype(BF16)
            inside = rel < 128
            kbuf[b] = jnp.where(inside, dot(hot, kcb[...]), kbuf[b].astype(F32)).astype(BF16)
            vbuf[b] = jnp.where(inside, dot(hot, vcb[...]), vbuf[b].astype(F32)).astype(BF16)

        for i, (src, dst) in enumerate(((kbuf, kn), (vbuf, vn))):
            cp = pltpu.make_async_copy(src.at[b], dst.at[b], out_sem.at[i, b])
            cp.start()
            writes.append(cp)
    for cp in writes:
        cp.wait()


def solution(mesh):
    row_spec = P('dp', 'tp', None)
    cache_spec = P('dp', None, 'tp', None)
    head_cols = P(None, 'tp', None)
    in_specs = (row_spec, P('dp'), cache_spec, cache_spec, P(), head_cols, head_cols, head_cols, P('tp', None, None), P(), P(None, 'tp'), P(None, 'tp'), P('tp', None))
    out_specs = (row_spec, cache_spec, cache_spec)

    def local_layer(x_in, start_pos, k_cache, v_cache, attn_gain, w_query, w_key, w_value, w_out, mlp_gain, w_gate, w_up, w_down):
        _, tb, D = x_in.shape
        T = 4 * tb
        window = k_cache.shape[1]
        F = w_gate.shape[1]
        HW = D // 2 // NCH
        CW = D // NCH2
        qh = w_query.shape[1]
        invf = jnp.asarray(np.repeat(ROPE_BASE ** (-np.arange(0, HD, 2) / HD), 2).astype(np.float32)[None])
        blocks = window // 128
        kc = k_cache.reshape(blocks, 256, HD)
        vc = v_cache.reshape(blocks, 256, HD)
        wk = w_key.reshape(D // 128, 256, HD)
        wv = w_value.reshape(D // 128, 256, HD)
        any_spec = pl.BlockSpec(memory_space=pl.ANY)
        vmem = pltpu.VMEM
        dma = pltpu.SemaphoreType.DMA
        x_out, k_ch, v_ch = pl.pallas_call(
            layer_kernel,
            name='layer',
            out_shape=(jax.ShapeDtypeStruct((tb, D), BF16), jax.ShapeDtypeStruct((2 * T, HD), BF16), jax.ShapeDtypeStruct((2 * T, HD), BF16)),
            in_specs=[any_spec] * 14,
            out_specs=(any_spec,) * 3,
            scratch_shapes=[
                pltpu.SMEM((1,), jnp.int32), vmem((1, HD), F32),
                vmem((tb, D), BF16), vmem((T, D // 2), BF16), vmem((T, D), BF16), vmem((D // HD, HD), BF16), vmem((D // HD, HD), BF16),
                vmem((blocks, 256, HD), BF16), vmem((blocks, 256, HD), BF16),
                vmem((qh, D, HD), BF16), vmem((D // 128, 256, HD), BF16), vmem((D // 128, 256, HD), BF16),
                vmem((qh * HD, D), BF16), vmem((D, F), BF16), vmem((D, F), BF16), vmem((F, D), BF16),
                vmem((5, T, 256), F32), vmem((8, window), jnp.int32),
                vmem((2, window // KB, 3 * T, KB), F32), vmem((2, 3 * T, HD), BF16), vmem((2, 128, HD), BF16), vmem((2, 128, HD), BF16),
                vmem((T, qh * HD), BF16),
                vmem((NCH, 2, T, HW), BF16), vmem((NCH, T, HW), BF16), vmem((NCH, T, HW), BF16), vmem((NCH, T, HW), BF16),
                vmem((NCH, 2, T, HW), BF16), vmem((2, T, F), F32), vmem((T, F), BF16),
                vmem((NCH2, 2, 2 * tb, CW), BF16), vmem((NCH2, 2 * tb, CW), BF16), vmem((NCH2, tb, CW), BF16), vmem((NCH2, tb, CW), BF16),
                vmem((tb, D), BF16), vmem((2 * T, HD), BF16), vmem((2 * T, HD), BF16),
                dma((15,)), dma((3,)), dma((1,)), dma((1,))] + [dma((NAG,))] * 4 + [dma((3,))] * 2 + [dma((NCH,))] * 6 + [dma((NCH2,))] * 4,
            compiler_params=pltpu.CompilerParams(collective_id=0, has_side_effects=True, vmem_limit_bytes=67043328),
        )(start_pos, invf, x_in.reshape(tb, D), attn_gain.reshape(D // HD, HD), mlp_gain.reshape(D // HD, HD), kc, vc, w_query.transpose(1, 0, 2), wk, wv,
          w_out.reshape(qh * HD, D), w_gate, w_up, w_down)
        nblk = 8
        per = 2 * window // nblk
        k_new, v_new, x_fin = pl.pallas_call(
            cache_kernel,
            name='cache',
            out_shape=(jax.ShapeDtypeStruct((nblk, per, HD), BF16),) * 2 + (jax.ShapeDtypeStruct((tb, D), BF16),),
            in_specs=[pl.BlockSpec(memory_space=pltpu.SMEM)] + [any_spec] * 5,
            out_specs=(any_spec,) * 3,
            scratch_shapes=[vmem((nblk, per, HD), BF16)] * 2 + [vmem((2 * T, HD), BF16)] * 2 + [vmem((tb, D), BF16), dma((3, nblk + 1)), dma((3, nblk))],
        )(start_pos, k_cache.reshape(nblk, per, HD), v_cache.reshape(nblk, per, HD), k_ch, v_ch, x_out)
        return x_fin.reshape(x_in.shape), k_new.reshape(k_cache.shape), v_new.reshape(v_cache.shape)

    return jax.shard_map(local_layer, mesh=mesh, in_specs=in_specs, out_specs=out_specs, check_vma=False)
```

```python
import functools

import jax
import jax.numpy as jnp
import numpy as np
from jax import lax
from jax.experimental import pallas as pl
from jax.experimental.pallas import tpu as pltpu
from jax.sharding import PartitionSpec as P

ROPE_BASE = 10000.0
NORM_EPS = 1e-5
MESH = pl.DeviceIdType.MESH
BF16 = jnp.bfloat16
F32 = jnp.float32
HD = 128
NCH = 6
NCH2 = 6
NAG = 4
LAG = 2
KB = 512
SLAB = 256
LAYER_VMEM = 62 * 10**6
CACHE_VMEM = 24 * 10**6
SPARE = 3 * 2**23


def dot(a, b):
    return jnp.dot(a, b, preferred_element_type=F32)


def dot_padded(a, b):
    p = dot(a, b)
    m = a.shape[0] // 2
    return p[:m] + p[m:]


def dot_t(a, b):
    return lax.dot_general(a, b, (((1,), (1,)), ((), ())), preferred_element_type=F32)


class Phases:
    def __init__(self):
        self.scope = None

    def __call__(self, name):
        self.close()
        self.scope = jax.named_scope(name)
        self.scope.__enter__()

    def close(self):
        if self.scope is not None:
            self.scope.__exit__(None, None, None)
        self.scope = None


def layer_kernel(start_hbm, invf_hbm, x_hbm, g1_hbm, g2_hbm, kc_hbm, vc_hbm, wq_hbm, wk_hbm, wv_hbm, wo_hbm, wg_hbm, wu_hbm, wd_hbm,
                 xo_hbm, kn_hbm, vn_hbm,
                 start_s, invf, xown, xh, nbuf, g1, g2, kbuf, vbuf, wq, wk, wv, wo, wg, wu, wd,
                 qacc, offb, sbuf, qbuf, kch, vch, obuf, part, rx1, cs, rx2, hbuf, gacc, ubuf, part2, rx4, cs2, rx5, xout, kout, vout,
                 ld_sem, st_sem, out_sem, agp_r, aga_r, agf_r, xs_r, r1, r2, r3, r4, r5):
    phase = Phases()
    phase('entry')
    T, D = nbuf.shape
    half = D // 2
    HW = half // NCH
    CW = D // NCH2
    AW = D // NAG
    tb = T // 4
    window = kbuf.shape[0] * 128
    F = wg.shape[0] * SLAB
    me = lax.axis_index('tp')
    core = lax.rem(me, 2)
    chip = lax.div(me, 2)
    partner = chip * 2 + (1 - core)
    across = (1 - chip) * 2 + core
    diag = (1 - chip) * 2 + (1 - core)

    def load(i, src, dst):
        return pltpu.make_async_copy(src, dst, ld_sem.at[i])

    def slabs(i, src, dst):
        return [load(i, src.at[:, j * SLAB:(j + 1) * SLAB], dst.at[j]) for j in range(dst.shape[0])]

    def cols(ref, rows, lo, n):
        parts = [ref[j, rows] for j in range(lo // SLAB, (lo + n) // SLAB)]
        return parts[0] if len(parts) == 1 else jnp.concatenate(parts, axis=1)

    def rows_of(owner):
        return pl.ds(pl.multiple_of(owner * tb, tb), tb)

    def half_of(which):
        return pl.ds(pl.multiple_of(which * half, 128), half)

    def remote(src, dst, recv, dev):
        return pltpu.make_async_remote_copy(src_ref=src, dst_ref=dst, send_sem=out_sem.at[0], recv_sem=recv, device_id={'tp': dev}, device_id_type=MESH)

    def wide(gain, lo, n):
        return jnp.concatenate([gain[i:i + 1] for i in range(lo // HD, (lo + n) // HD)], axis=1)

    barrier = pltpu.get_barrier_semaphore()
    for other in (across, diag, partner):
        pl.semaphore_signal(barrier, inc=1, device_id={'tp': other}, device_id_type=MESH)

    own = rows_of(me)
    ld_x = [load(0, x_hbm, xown), load(0, g1_hbm, g1)]
    ld_small = [load(1, g2_hbm, g2), load(1, start_hbm, start_s), load(1, invf_hbm, invf), load(1, x_hbm.at[:, half_of(core)], xh.at[own])]
    ld_cache = [load(2, kc_hbm, kbuf), load(2, vc_hbm, vbuf)]
    ld_wkv = [load(3, wk_hbm, wk), load(3, wv_hbm, wv)]
    ld_wq = [load(4, wq_hbm, wq)]
    ld_wo = slabs(5, wo_hbm, wo)
    ld_gu = slabs(6, wg_hbm, wg) + slabs(6, wu_hbm, wu)
    n_main = wd.shape[0]
    wd_slabs = [wd.at[j] if j < n_main else wq.at[pl.ds((j - n_main) * F, F)] for j in range(D // HD)]
    ld_wd = [load(7, wd_hbm.at[:, j * HD:(j + 1) * HD], wd_slabs[j]) for j in range(D // HD)]

    def wd_cols(lo, n):
        return jnp.concatenate([wd_slabs[j][...] for j in range(lo // HD, (lo + n) // HD)], axis=1)

    def wait(group):
        for item in group:
            item.wait()

    for item in ld_x + ld_small + ld_cache + ld_wkv + ld_wq + ld_wo + ld_gu + ld_wd[:n_main]:
        item.start()

    wait(ld_x)
    x32 = xown[...].astype(F32)
    inv = lax.rsqrt(jnp.mean(x32 * x32, axis=-1, keepdims=True) + NORM_EPS)
    nbuf[own] = (x32 * inv * wide(g1[...].astype(F32), 0, D)).astype(BF16)
    pl.semaphore_wait(barrier, 3)
    ag_a = []
    for c in range(NAG):
        piece = nbuf.at[own, pl.ds(c * AW, AW)]
        ag_a.append(remote(piece, piece, aga_r.at[c], across))
        ag_a[c].start()
    ag_p = remote(nbuf.at[own], nbuf.at[own], agp_r.at[0], partner)
    ag_p.start()

    row = lax.broadcasted_iota(jnp.int32, (256, 256), 0)
    col = lax.broadcasted_iota(jnp.int32, (256, 256), 1)
    pick = jnp.where(col == 2 * lax.rem(row, 128) + lax.div(row, 128), 1.0, 0.0).astype(BF16)

    def split(a_ref, b_ref, lo, hi):
        def body(b, carry):
            both = jnp.concatenate([a_ref[b], b_ref[b]], axis=1)
            sep = dot(pick, both).astype(BF16)
            a_ref[b] = sep[:, :128]
            b_ref[b] = sep[:, 128:]
            return carry
        lax.fori_loop(lo, hi, body, 0, unroll=min(8, hi - lo))

    phase('wait_cache')
    wait(ld_cache)
    phase('split_cache')
    split(kbuf, vbuf, 0, kbuf.shape[0])
    phase('wait_wkv')
    wait(ld_wkv)
    ag_f = []
    per_ag = wk.shape[0] // NAG
    for c in range(NAG):
        phase(f'wait_across{c}')
        ag_a[c].wait_recv()
        piece = nbuf.at[rows_of(across), pl.ds(c * AW, AW)]
        ag_f.append(remote(piece, piece, agf_r.at[c], partner))
        ag_f[c].start()
        phase(f'split_wkv{c}')
        split(wk, wv, c * per_ag, (c + 1) * per_ag)

    x_sends = [remote(xown.at[:, half_of(core)], xh.at[own], xs_r.at[0], across),
               remote(xown.at[:, half_of(1 - core)], xh.at[own], xs_r.at[1], diag),
               remote(xown.at[:, half_of(1 - core)], xh.at[own], xs_r.at[2], partner)]
    for cp in x_sends:
        cp.start()

    phase('trig')
    wait(ld_small)
    start = start_s[0]
    lane = lax.broadcasted_iota(jnp.int32, (T, HD), 1)
    tok = lax.broadcasted_iota(jnp.int32, (T, HD), 0)
    angles = (start + tok).astype(F32) * invf[...]
    cos_t = jnp.cos(angles)
    even = lax.rem(lane, 2) == 0
    sin_t = jnp.sin(angles)
    sin_t = jnp.where(even, -sin_t, sin_t)
    slot = lax.broadcasted_iota(jnp.int32, (8, window), 1)
    off = lax.rem(slot - start + 4 * window, window)
    offb[...] = jnp.where(start - window + off >= 0, off, -1)

    def rope(h):
        swapped = jnp.where(even, pltpu.roll(h, HD - 1, 1), pltpu.roll(h, 1, 1))
        return h * cos_t + swapped * sin_t

    def split_rows(ref, g, c):
        return ref[c * per_ag:(c + 1) * per_ag, g * 128:(g + 1) * 128, :].reshape(AW, HD)

    ag_p.wait_recv()
    wait(ld_wq)
    ubuf[T:] = jnp.zeros((T, F), BF16)
    kch[...] = jnp.zeros_like(kch)
    vch[...] = jnp.zeros_like(vch)
    for c in range(NAG):
        phase(f'wait_fwd{c}')
        ag_f[c].wait_recv()
        phase(f'qkv{c}')
        rows = nbuf[:, c * AW:(c + 1) * AW]
        for o in range(5):
            if o < 3:
                w = jnp.concatenate([wq[h * D + c * AW:h * D + (c + 1) * AW] for h in (2 * o, 2 * o + 1)], axis=1)
            else:
                ref = wk if o == 3 else wv
                w = jnp.concatenate([split_rows(ref, 0, c), split_rows(ref, 1, c)], axis=1)
            p = dot(rows, w)
            qacc[o] = p if c == 0 else qacc[o] + p
    phase('rope')
    for item in ld_wd[n_main:]:
        item.start()
    for g in range(2):
        kch[g, :T] = rope(qacc[3, :, g * HD:(g + 1) * HD]).astype(BF16)
        vch[g, :T] = qacc[4, :, g * HD:(g + 1) * HD].astype(BF16)
    for head in range(6):
        qbuf[head // 3, (head % 3) * T:(head % 3 + 1) * T] = rope(qacc[head // 2, :, (head % 2) * HD:(head % 2 + 1) * HD]).astype(BF16)

    phase('attn')
    coef = HD ** -0.5 * float(np.log2(np.e))
    nblk = window // KB
    nb = KB // 128
    q_tok = lax.broadcasted_iota(jnp.int32, (T, HD), 0)
    q_tok3 = q_tok.reshape(T // 8, 8, HD)
    k_idx = lax.broadcasted_iota(jnp.int32, (T, HD), 1)

    def blocks(ref, g, i):
        return ref[i * nb:(i + 1) * nb, g * 128:(g + 1) * 128, :].reshape(KB, HD)

    top, mass, s_c = [[None] * 3, [None] * 3], [[None] * 3, [None] * 3], [[None] * 3, [None] * 3]
    peak, e_c, scale, acc = [[None] * 3, [None] * 3], [[None] * 3, [None] * 3], [[None] * 3, [None] * 3], [None, None]

    def score_chunk(g):
        s = dot_t(qbuf[g], kch[g])
        for h in range(3):
            s_c[g][h] = jnp.where(k_idx <= q_tok, s[h * T:(h + 1) * T], -jnp.inf)
            top[g][h] = s_c[g][h]

    def score(g, i):
        s = dot_t(qbuf[g], blocks(kbuf, g, i))
        for j in range(nb):
            o = offb[:, i * KB + j * 128:i * KB + (j + 1) * 128][None]
            keep = o > q_tok3
            for h in range(3):
                piece = s[h * T:(h + 1) * T, j * 128:(j + 1) * 128].reshape(T // 8, 8, HD)
                piece = jnp.where(keep, piece, -jnp.inf).reshape(T, HD)
                sbuf[g, i, h * T:(h + 1) * T, j * 128:(j + 1) * 128] = piece
                top[g][h] = jnp.maximum(top[g][h], piece)

    def expo_chunk(g):
        for h in range(3):
            peak[g][h] = jnp.max(top[g][h], axis=1, keepdims=True)
            e_c[g][h] = jnp.exp2((s_c[g][h] - peak[g][h]) * coef)
            mass[g][h] = e_c[g][h]

    def expo(g, h, i):
        e = jnp.exp2((sbuf[g, i, h * T:(h + 1) * T] - peak[g][h]) * coef)
        sbuf[g, i, h * T:(h + 1) * T] = e
        for j in range(nb):
            mass[g][h] = mass[g][h] + e[:, j * 128:(j + 1) * 128]

    def weigh_chunk(g):
        for h in range(3):
            scale[g][h] = 1.0 / jnp.sum(mass[g][h], axis=1, keepdims=True)
        p = jnp.concatenate([(e_c[g][h] * scale[g][h]).astype(BF16) for h in range(3)], axis=0)
        acc[g] = dot(p, vch[g])

    def weigh(g, i):
        p = jnp.concatenate([(sbuf[g, i, h * T:(h + 1) * T] * scale[g][h]).astype(BF16) for h in range(3)], axis=0)
        acc[g] = acc[g] + dot(p, blocks(vbuf, g, i))

    order = [(h, i) for h in range(3) for i in range(nblk)]
    score_chunk(0)
    for i in range(nblk):
        score(0, i)
    score_chunk(1)
    expo_chunk(0)
    for i in range(nblk):
        score(1, i)
        for h, k in order[3 * i:3 * i + 3]:
            expo(0, h, k)
    expo_chunk(1)
    weigh_chunk(0)
    for i in range(nblk):
        weigh(0, i)
        for h, k in order[3 * i:3 * i + 3]:
            expo(1, h, k)
    weigh_chunk(1)
    for i in range(nblk):
        weigh(1, i)
    for g in range(2):
        for h in range(3):
            head = 3 * g + h
            obuf[:, head * HD:(head + 1) * HD] = acc[g][h * T:(h + 1) * T].astype(BF16)

    phase('oproj')
    wait(ld_wo)
    hop1, hop2, hop3, hop4, hop5 = [], [], [], [], []
    def out_chunk(c):
        return [dot(obuf[...], cols(wo, slice(None), i * half + c * HW, HW)) for i in range(2)]

    ready = out_chunk(0)
    for c in range(NCH):
        now, ready = ready, out_chunk(c + 1) if c + 1 < NCH else None
        for i in range(2):
            part[c, i] = now[i].astype(BF16)
        hop1.append(remote(part.at[c, 1 - core], rx1.at[c], r1.at[c], partner))
        hop1[c].start()
    phase('hop1')
    for c in range(NCH):
        hop1[c].wait_recv()
        cs[c] = (part[c, core].astype(F32) + rx1[c].astype(F32)).astype(BF16)
        hop2.append(remote(cs.at[c], rx2.at[c], r2.at[c], across))
        hop2[c].start()

    phase('kvout')
    prow = lax.broadcasted_iota(jnp.int32, (2 * T, HD), 0)
    pcol = lax.broadcasted_iota(jnp.int32, (2 * T, HD), 1)
    for src, dst in ((kch, kout), (vch, vout)):
        mix = sum(dot(jnp.where(prow == 2 * pcol + g, 1.0, 0.0).astype(BF16), src[g]) for g in range(2))
        dst[...] = mix.astype(BF16)
    store_k = pltpu.make_async_copy(kout, kn_hbm.at[:2 * T], st_sem.at[0])
    store_v = pltpu.make_async_copy(vout, vn_hbm.at[:2 * T], st_sem.at[0])
    store_k.start()
    store_v.start()

    phase('hop2')
    for cp in x_sends:
        cp.wait_recv()
    gain2 = g2[...].astype(F32)
    g_top = jnp.maximum(jnp.max(jnp.max(jnp.abs(gain2), axis=1, keepdims=True), axis=0, keepdims=True), 1e-30)
    gain2 = gain2 / g_top
    wait(ld_gu)
    squares = []

    def gate_up(c):
        hop3[c].wait_recv()
        phase(f'gateup{c}')
        lhs = []
        for i in range(2):
            h32 = hbuf[c, i].astype(F32)
            lhs.append(jnp.concatenate([(h32 * wide(gain2, i * half + c * HW, HW)).astype(BF16), jnp.zeros((T, HW), BF16)], axis=0))
            for j in range(HW // 128):
                piece = h32[:, j * 128:(j + 1) * 128]
                squares.append(piece * piece if not squares else squares.pop() + piece * piece)
        for k, w in enumerate((wg, wu)):
            for lo in range(0, F, 512):
                p = sum(dot_padded(lhs[i], cols(w, slice(i * half + c * HW, i * half + (c + 1) * HW), lo, 512)) for i in range(2))
                gacc[k, :, lo:lo + 512] = p if c == 0 else gacc[k, :, lo:lo + 512] + p

    for c in range(NCH):
        phase(f'hop2_{c}')
        hop2[c].wait_recv()
        total = cs[c].astype(F32) + rx2[c].astype(F32)
        hbuf[c, core] = (xh[:, c * HW:(c + 1) * HW].astype(F32) + total).astype(BF16)
        hop3.append(remote(hbuf.at[c, core], hbuf.at[c, core], r3.at[c], partner))
        hop3[c].start()
        if c >= 2:
            gate_up(c - 2)
    for c in range(NCH - 2, NCH):
        phase(f'hop3_{c}')
        gate_up(c)
    phase('act')
    inv2 = lax.rsqrt(jnp.sum(squares[0], axis=-1, keepdims=True) / D + NORM_EPS)
    inv2 = inv2 * g_top
    gate = jnp.where(inv2 > 0, gacc[0] * inv2, 0.0)
    up = jnp.where(inv2 > 0, gacc[1] * inv2, 0.0)
    ubuf[:T] = (gate * jax.nn.sigmoid(gate) * up).astype(BF16)

    phase('down')
    wait(ld_wd)
    mine = rows_of(chip)
    theirs = rows_of(1 - chip)

    def chip_sum(c):
        hop4[c].wait_recv()
        cs2[c] = (part2[c, core, theirs].astype(F32) + rx4[c, theirs].astype(F32)).astype(BF16)
        hop5.append(remote(cs2.at[c], rx5.at[c], r5.at[c], across))
        hop5[c].start()

    def down_chunk(c):
        return dot_padded(ubuf[...], wd_cols(c * CW, CW))

    ready = down_chunk(0)
    for c in range(NCH2):
        p, ready = ready.astype(BF16), down_chunk(c + 1) if c + 1 < NCH2 else None
        for o in range(4):
            part2[c, o % 2, (o // 2) * tb:(o // 2 + 1) * tb] = p[o * tb:(o + 1) * tb]
        hop4.append(remote(part2.at[c, 1 - core], rx4.at[c], r4.at[c], partner))
        hop4[c].start()
        if c >= LAG:
            chip_sum(c - LAG)
    phase('hop4')
    for c in range(NCH2 - LAG, NCH2):
        chip_sum(c)
    phase('hop5')
    for c in range(NCH2):
        hop5[c].wait_recv()
        local = part2[c, core, mine].astype(F32) + rx4[c, mine].astype(F32) + rx5[c].astype(F32)
        for j in range(CW // HW):
            lo = c * CW + j * HW
            h_own = hbuf[(lo % half) // HW, lo // half, own].astype(F32)
            xout[:, lo:lo + HW] = (h_own + local[:, j * HW:(j + 1) * HW]).astype(BF16)
    store_x = pltpu.make_async_copy(xout, xo_hbm.at[:tb], st_sem.at[0])
    phase('fin')
    store_x.start()
    for cp in ag_a + [ag_p] + ag_f + x_sends + hop1 + hop2 + hop3 + hop4 + hop5:
        cp.wait_send()
    store_k.wait()
    store_v.wait()
    store_x.wait()
    phase.close()


def cache_kernel(start_ref, kc, vc, kch, vch, xin, kn, vn, xo, kbuf, vbuf, kcb, vcb, xb, in_sem, out_sem):
    nblk, per, _ = kc.shape
    rows = nblk * per
    small = [pltpu.make_async_copy(src, dst, in_sem.at[0]) for src, dst in ((kch.at[:kcb.shape[0]], kcb), (vch.at[:vcb.shape[0]], vcb), (xin.at[:xb.shape[0]], xb))]
    for cp in small:
        cp.start()
    first = lax.rem(2 * start_ref[0], rows)
    jrow = lax.broadcasted_iota(jnp.int32, (per, 128), 0)
    jcol = lax.broadcasted_iota(jnp.int32, (per, 128), 1)

    def touched(b):
        ahead = lax.rem(b * per - first + rows, rows)
        return (ahead < 128) | (ahead > rows - per)

    def writes(b, k_src, v_src):
        return [pltpu.make_async_copy(k_src.at[b], kn.at[b], out_sem.at[0]), pltpu.make_async_copy(v_src.at[b], vn.at[b], out_sem.at[0])]

    for b in range(nblk):
        @pl.when(jnp.logical_not(touched(b)))
        def _():
            for cp in writes(b, kc, vc):
                cp.start()

    for cp in small:
        cp.wait()
    x_write = pltpu.make_async_copy(xb, xo, out_sem.at[0])
    x_write.start()
    for b in range(nblk):
        @pl.when(touched(b))
        def _():
            rel = lax.rem(jrow + b * per - first + rows, rows)
            hot = jnp.where(rel == jcol, 1.0, 0.0).astype(BF16)
            inside = rel < 128
            kbuf[b] = jnp.where(inside, dot(hot, kcb[...]), kc[b].astype(F32)).astype(BF16)
            vbuf[b] = jnp.where(inside, dot(hot, vcb[...]), vc[b].astype(F32)).astype(BF16)
            for cp in writes(b, kbuf, vbuf):
                cp.start()

    x_write.wait()
    for b in range(nblk):
        for cp in writes(b, kbuf, vbuf):
            cp.wait()


def solution(mesh):
    row_spec = P('dp', 'tp', None)
    cache_spec = P('dp', None, 'tp', None)
    head_cols = P(None, 'tp', None)
    in_specs = (row_spec, P('dp'), cache_spec, cache_spec, P(), head_cols, head_cols, head_cols, P('tp', None, None), P(), P(None, 'tp'), P(None, 'tp'), P('tp', None))
    out_specs = (row_spec, cache_spec, cache_spec)

    def local_layer(x_in, start_pos, k_cache, v_cache, attn_gain, w_query, w_key, w_value, w_out, mlp_gain, w_gate, w_up, w_down):
        _, tb, D = x_in.shape
        T = 4 * tb
        window = k_cache.shape[1]
        F = w_gate.shape[1]
        HW = D // 2 // NCH
        CW = D // NCH2
        qh = w_query.shape[1]
        invf = jnp.asarray(np.repeat(ROPE_BASE ** (-np.arange(0, HD, 2) / HD), 2).astype(np.float32)[None])
        blocks = window // 128
        kc = k_cache.reshape(blocks, 256, HD)
        vc = v_cache.reshape(blocks, 256, HD)
        wk = w_key.reshape(D // 128, 256, HD)
        wv = w_value.reshape(D // 128, 256, HD)
        any_spec = pl.BlockSpec(memory_space=pl.ANY)
        vmem = pltpu.VMEM
        dma = pltpu.SemaphoreType.DMA
        x_out, k_ch, v_ch = pl.pallas_call(
            layer_kernel,
            name='layer',
            out_shape=(jax.ShapeDtypeStruct((SPARE // D, D), BF16), jax.ShapeDtypeStruct((SPARE // HD, HD), BF16), jax.ShapeDtypeStruct((SPARE // HD, HD), BF16)),
            in_specs=[any_spec] * 14,
            out_specs=(any_spec,) * 3,
            scratch_shapes=[
                pltpu.SMEM((1,), jnp.int32), vmem((1, HD), F32),
                vmem((tb, D), BF16), vmem((T, D // 2), BF16), vmem((T, D), BF16), vmem((D // HD, HD), BF16), vmem((D // HD, HD), BF16),
                vmem((blocks, 256, HD), BF16), vmem((blocks, 256, HD), BF16),
                vmem((qh * D, HD), BF16), vmem((D // 128, 256, HD), BF16), vmem((D // 128, 256, HD), BF16),
                vmem((D // SLAB, qh * HD, SLAB), BF16), vmem((F // SLAB, D, SLAB), BF16), vmem((F // SLAB, D, SLAB), BF16), vmem((D // HD - qh * D // F, F, HD), BF16),
                vmem((5, T, 256), F32), vmem((8, window), jnp.int32),
                vmem((2, window // KB, 3 * T, KB), F32), vmem((2, 3 * T, HD), BF16), vmem((2, 128, HD), BF16), vmem((2, 128, HD), BF16),
                vmem((T, qh * HD), BF16),
                vmem((NCH, 2, T, HW), BF16), vmem((NCH, T, HW), BF16), vmem((NCH, T, HW), BF16), vmem((NCH, T, HW), BF16),
                vmem((NCH, 2, T, HW), BF16), vmem((2, T, F), F32), vmem((2 * T, F), BF16),
                vmem((NCH2, 2, 2 * tb, CW), BF16), vmem((NCH2, 2 * tb, CW), BF16), vmem((NCH2, tb, CW), BF16), vmem((NCH2, tb, CW), BF16),
                vmem((tb, D), BF16), vmem((2 * T, HD), BF16), vmem((2 * T, HD), BF16),
                dma((8,)), dma((1,)), dma((1,)), dma((1,))] + [dma((NAG,))] * 2 + [dma((3,))] + [dma((NCH,))] * 3 + [dma((NCH2,))] * 2,
            compiler_params=pltpu.CompilerParams(collective_id=0, has_side_effects=True, vmem_limit_bytes=LAYER_VMEM),
            cost_estimate=pl.CostEstimate(flops=2 * 64 * 25 * 10**6, bytes_accessed=80 * 10**6, transcendentals=3 * 10**6),
        )(start_pos, invf, x_in.reshape(tb, D), attn_gain.reshape(D // HD, HD), mlp_gain.reshape(D // HD, HD), kc, vc, w_query.transpose(1, 0, 2).reshape(qh * D, HD), wk, wv,
          w_out.reshape(qh * HD, D), w_gate, w_up, w_down)
        nblk = 16
        per = 2 * window // nblk
        k_new, v_new, x_fin = pl.pallas_call(
            cache_kernel,
            name='cache',
            out_shape=(jax.ShapeDtypeStruct((nblk, per, HD), BF16),) * 2 + (jax.ShapeDtypeStruct((tb, D), BF16),),
            in_specs=[pl.BlockSpec(memory_space=pltpu.SMEM)] + [pl.BlockSpec(memory_space=pltpu.VMEM)] * 2 + [pl.BlockSpec(memory_space=pltpu.HBM)] * 3,
            out_specs=(any_spec,) * 3,
            scratch_shapes=[vmem((nblk, per, HD), BF16)] * 2 + [vmem((2 * T, HD), BF16)] * 2 + [vmem((tb, D), BF16), dma((1,)), dma((1,))],
            compiler_params=pltpu.CompilerParams(vmem_limit_bytes=CACHE_VMEM),
        )(start_pos, k_cache.reshape(nblk, per, HD), v_cache.reshape(nblk, per, HD), k_ch, v_ch, x_out)
        return x_fin.reshape(x_in.shape), k_new.reshape(k_cache.shape), v_new.reshape(v_cache.shape)

    return jax.shard_map(local_layer, mesh=mesh, in_specs=in_specs, out_specs=out_specs, check_vma=False)
```

```python
import functools

import jax
import jax.numpy as jnp
import numpy as np
from jax import lax
from jax.experimental import pallas as pl
from jax.experimental.pallas import tpu as pltpu
from jax.sharding import PartitionSpec as P

ROPE_BASE = 10000.0
NORM_EPS = 1e-5
MESH = pl.DeviceIdType.MESH
BF16 = jnp.bfloat16
F32 = jnp.float32
HD = 128
OUT_W = (256, 256, 256, 256, 256, 256)
OUT_LO = tuple(sum(OUT_W[:i]) for i in range(len(OUT_W)))
NCH = len(OUT_W)
OUT_GROUPS = ((0,), (1, 2), (3, 4, 5))
DOWN = (0, 1024, 2048, 2560, 3072)
NAG = 4
LAG = 2
GLAG = 2
KB = 512
SLAB = 256
LAYER_VMEM = 62600000
CACHE_VMEM = 24 * 10**6
SPARE = 3 * 2**23


def dot(a, b):
    return jnp.dot(a, b, preferred_element_type=F32)


def dot_padded(a, b):
    p = dot(a, b)
    m = a.shape[0] // 2
    return p[:m] + p[m:]


def dot_t(a, b):
    return lax.dot_general(a, b, (((1,), (1,)), ((), ())), preferred_element_type=F32)


class Phases:
    def __init__(self):
        self.scope = None

    def __call__(self, name):
        self.close()
        self.scope = jax.named_scope(name)
        self.scope.__enter__()

    def close(self):
        if self.scope is not None:
            self.scope.__exit__(None, None, None)
        self.scope = None


def layer_kernel(start_hbm, invf_hbm, x_hbm, g1_hbm, g2_hbm, kc_hbm, vc_hbm, wq_hbm, wk_hbm, wv_hbm, wo_hbm, wg_hbm, wu_hbm, wd_hbm,
                 xo_hbm, kn_hbm, vn_hbm,
                 start_s, invf, xown, xh, nbuf, g1, g2, kbuf, vbuf, wq, wk, wv, wo, wg, wu, wd,
                 qacc, offb, sbuf, qbuf, kch, vch, obuf, part, rx1, cs, rx2, hbuf, gacc, ubuf, part2, rx4, cs2, rx5, xout, kout, vout,
                 ld_sem, st_sem, out_sem, agp_r, aga_r, xs_r, r1, r2, r3, r5):
    phase = Phases()
    phase('entry')
    T, D = nbuf.shape
    half = D // 2
    AW = D // NAG
    tb = T // 4
    window = kbuf.shape[0] * 128
    F = wg.shape[0] * SLAB
    me = lax.axis_index('tp')
    core = lax.rem(me, 2)
    chip = lax.div(me, 2)
    partner = chip * 2 + (1 - core)
    across = (1 - chip) * 2 + core
    diag = (1 - chip) * 2 + (1 - core)

    def load(i, src, dst):
        return pltpu.make_async_copy(src, dst, ld_sem.at[i])

    def slabs(i, src, dst):
        return [load(i, src.at[:, j * SLAB:(j + 1) * SLAB], dst.at[j]) for j in range(dst.shape[0])]

    def cols(ref, rows, lo, n):
        parts = [ref[j * HD // SLAB, rows, j * HD % SLAB:j * HD % SLAB + HD] for j in range(lo // HD, (lo + n) // HD)]
        return parts[0] if len(parts) == 1 else jnp.concatenate(parts, axis=1)

    def span(c):
        return slice(OUT_LO[c], OUT_LO[c] + OUT_W[c])

    def rows_of(owner):
        return pl.ds(pl.multiple_of(owner * tb, tb), tb)

    def half_of(which):
        return pl.ds(pl.multiple_of(which * half, 128), half)

    def remote(src, dst, recv, dev):
        return pltpu.make_async_remote_copy(src_ref=src, dst_ref=dst, send_sem=out_sem.at[0], recv_sem=recv, device_id={'tp': dev}, device_id_type=MESH)

    def wide(gain, lo, n):
        return jnp.concatenate([gain[i:i + 1] for i in range(lo // HD, (lo + n) // HD)], axis=1)

    barrier = pltpu.get_barrier_semaphore()
    for other in (across, diag, partner):
        pl.semaphore_signal(barrier, inc=1, device_id={'tp': other}, device_id_type=MESH)

    own = rows_of(me)
    ld_x = [load(0, x_hbm, xown), load(0, g1_hbm, g1)]
    ld_small = [load(1, g2_hbm, g2), load(1, start_hbm, start_s), load(1, invf_hbm, invf), load(1, x_hbm.at[:, half_of(core)], xh.at[own])]
    ld_cache = [load(2, kc_hbm, kbuf), load(2, vc_hbm, vbuf)]
    ld_wkv = [load(3, wk_hbm, wk), load(3, wv_hbm, wv)]
    ld_wq = [load(4, wq_hbm, wq)]
    ld_wo = slabs(5, wo_hbm, wo)
    ld_gu = slabs(6, wg_hbm, wg) + slabs(6, wu_hbm, wu)
    n_main = wd.shape[0]
    wd_slabs = [wd.at[j] if j < n_main else wq.at[pl.ds((j - n_main) * F, F)] for j in range(D // HD)]
    ld_wd = [load(7, wd_hbm.at[:, j * HD:(j + 1) * HD], wd_slabs[j]) for j in range(D // HD)]

    def wd_cols(lo, n):
        return jnp.concatenate([wd_slabs[j][...] for j in range(lo // HD, (lo + n) // HD)], axis=1)

    def wait(group):
        for item in group:
            item.wait()

    for item in ld_x + ld_small + ld_cache + ld_wkv + ld_wq + ld_wo + ld_gu + ld_wd[:n_main]:
        item.start()

    wait(ld_x)
    x32 = xown[...].astype(F32)
    inv = lax.rsqrt(jnp.mean(x32 * x32, axis=-1, keepdims=True) + NORM_EPS)
    nbuf[own] = (x32 * inv * wide(g1[...].astype(F32), 0, D)).astype(BF16)
    pl.semaphore_wait(barrier, 3)
    ag_a = []
    for c in range(NAG):
        piece = nbuf.at[own, pl.ds(c * AW, AW)]
        ag_a.append(remote(piece, piece, aga_r.at[c], across))
        ag_a[c].start()
    ag_p = remote(nbuf.at[own], nbuf.at[own], agp_r.at[0], partner)
    ag_p.start()

    phase('trig')
    wait(ld_small)
    start = start_s[0]
    lane = lax.broadcasted_iota(jnp.int32, (T, HD), 1)
    tok = lax.broadcasted_iota(jnp.int32, (T, HD), 0)
    angles = (start + tok).astype(F32) * invf[...]
    cos_t = jnp.cos(angles)
    even = lax.rem(lane, 2) == 0
    sin_t = jnp.sin(angles)
    sin_t = jnp.where(even, -sin_t, sin_t)
    slot = lax.broadcasted_iota(jnp.int32, (8, window), 1)
    off = lax.rem(slot - start + 4 * window, window)
    offb[...] = jnp.where(start - window + off >= 0, off, -1)

    def rope(h):
        swapped = jnp.where(even, pltpu.roll(h, HD - 1, 1), pltpu.roll(h, 1, 1))
        return h * cos_t + swapped * sin_t

    row = lax.broadcasted_iota(jnp.int32, (256, 256), 0)
    col = lax.broadcasted_iota(jnp.int32, (256, 256), 1)
    pick = jnp.where(col == 2 * lax.rem(row, 128) + lax.div(row, 128), 1.0, 0.0).astype(BF16)

    def split(a_ref, b_ref, lo, hi):
        def body(b, carry):
            both = jnp.concatenate([a_ref[b], b_ref[b]], axis=1)
            sep = dot(pick, both).astype(BF16)
            a_ref[b] = sep[:, :128]
            b_ref[b] = sep[:, 128:]
            return carry
        lax.fori_loop(lo, hi, body, 0, unroll=12 if (hi - lo) % 12 == 0 else 16)

    phase('wait_cache')
    wait(ld_cache)
    phase('split_cache')
    split(kbuf, vbuf, 0, kbuf.shape[0])
    phase('wait_wkv')
    wait(ld_wkv)
    ag_f = []

    def relay(c):
        ag_a[c].wait_recv()
        piece = nbuf.at[rows_of(across), pl.ds(c * AW, AW)]
        ag_f.append(remote(piece, piece, r3.at[c], partner))
        ag_f[c].start()

    phase('split_wkv')
    split(wk, wv, 0, wk.shape[0])
    for c in range(NAG):
        phase(f'wait_across{c}')
        relay(c)

    QW = AW
    per_q = QW // 128

    def split_rows(ref, g, c):
        return ref[c * per_q:(c + 1) * per_q, g * 128:(g + 1) * 128, :].reshape(QW, HD)

    ag_p.wait_recv()
    wait(ld_wq)
    ubuf[T:] = jnp.zeros((T, F), BF16)
    kch[...] = jnp.zeros_like(kch)
    vch[...] = jnp.zeros_like(vch)
    for c in range(NAG):
        phase(f'wait_fwd{c}')
        ag_f[c].wait_recv()
        phase(f'qkv{c}')
        rows = nbuf[:, c * QW:(c + 1) * QW]
        for o in range(5):
            if o < 3:
                w = jnp.concatenate([wq[h * D + c * QW:h * D + (c + 1) * QW] for h in (2 * o, 2 * o + 1)], axis=1)
            else:
                ref = wk if o == 3 else wv
                w = jnp.concatenate([split_rows(ref, 0, c), split_rows(ref, 1, c)], axis=1)
            p = dot(rows, w)
            qacc[o] = p if c == 0 else qacc[o] + p
    phase('rope')
    x_sends = [remote(xown.at[:, half_of(core)], xh.at[own], xs_r.at[0], across),
               remote(xown.at[:, half_of(1 - core)], xh.at[own], xs_r.at[1], diag),
               remote(xown.at[:, half_of(1 - core)], xh.at[own], xs_r.at[2], partner)]
    for cp in x_sends:
        cp.start()

    for item in ld_wd[n_main:]:
        item.start()
    for g in range(2):
        kch[g, :T] = rope(qacc[3, :, g * HD:(g + 1) * HD]).astype(BF16)
        vch[g, :T] = qacc[4, :, g * HD:(g + 1) * HD].astype(BF16)
    for head in range(6):
        qbuf[head // 3, (head % 3) * T:(head % 3 + 1) * T] = rope(qacc[head // 2, :, (head % 2) * HD:(head % 2 + 1) * HD]).astype(BF16)

    phase('attn')
    coef = HD ** -0.5 * float(np.log2(np.e))
    nblk = window // KB
    nb = KB // 128
    q_tok = lax.broadcasted_iota(jnp.int32, (T, HD), 0)
    q_tok3 = q_tok.reshape(T // 8, 8, HD)
    k_idx = lax.broadcasted_iota(jnp.int32, (T, HD), 1)

    def blocks(ref, g, i):
        return ref[i * nb:(i + 1) * nb, g * 128:(g + 1) * 128, :].reshape(KB, HD)

    top, mass, s_c = [[None] * 3, [None] * 3], [[None] * 3, [None] * 3], [[None] * 3, [None] * 3]
    peak, e_c, scale, acc = [[None] * 3, [None] * 3], [[None] * 3, [None] * 3], [[None] * 3, [None] * 3], [None, None]

    def score_chunk(g):
        s = dot_t(qbuf[g], kch[g])
        for h in range(3):
            s_c[g][h] = jnp.where(k_idx <= q_tok, s[h * T:(h + 1) * T], -jnp.inf)
            top[g][h] = s_c[g][h]

    def score(g, i):
        s = dot_t(qbuf[g], blocks(kbuf, g, i))
        for j in range(nb):
            o = offb[:, i * KB + j * 128:i * KB + (j + 1) * 128][None]
            keep = o > q_tok3
            for h in range(3):
                piece = s[h * T:(h + 1) * T, j * 128:(j + 1) * 128].reshape(T // 8, 8, HD)
                piece = jnp.where(keep, piece, -jnp.inf).reshape(T, HD)
                sbuf[g, i, h * T:(h + 1) * T, j * 128:(j + 1) * 128] = piece
                top[g][h] = jnp.maximum(top[g][h], piece)

    def expo_chunk(g):
        for h in range(3):
            peak[g][h] = jnp.max(top[g][h], axis=1, keepdims=True)
            e_c[g][h] = jnp.exp2((s_c[g][h] - peak[g][h]) * coef)
            mass[g][h] = e_c[g][h]

    def expo(g, h, i):
        e = jnp.exp2((sbuf[g, i, h * T:(h + 1) * T] - peak[g][h]) * coef)
        sbuf[g, i, h * T:(h + 1) * T] = e
        for j in range(nb):
            mass[g][h] = mass[g][h] + e[:, j * 128:(j + 1) * 128]

    def weigh_chunk(g):
        for h in range(3):
            scale[g][h] = 1.0 / jnp.sum(mass[g][h], axis=1, keepdims=True)
        p = jnp.concatenate([(e_c[g][h] * scale[g][h]).astype(BF16) for h in range(3)], axis=0)
        acc[g] = dot(p, vch[g])

    def weigh(g, i):
        p = jnp.concatenate([(sbuf[g, i, h * T:(h + 1) * T] * scale[g][h]).astype(BF16) for h in range(3)], axis=0)
        acc[g] = acc[g] + dot(p, blocks(vbuf, g, i))

    order = [(h, i) for h in range(3) for i in range(nblk)]
    score_chunk(0)
    for i in range(nblk):
        score(0, i)
    score_chunk(1)
    expo_chunk(0)
    for i in range(nblk):
        score(1, i)
        for h, k in order[3 * i:3 * i + 3]:
            expo(0, h, k)
    expo_chunk(1)
    weigh_chunk(0)
    for i in range(nblk):
        weigh(0, i)
        for h, k in order[3 * i:3 * i + 3]:
            expo(1, h, k)
    weigh_chunk(1)
    for i in range(nblk):
        weigh(1, i)
    for g in range(2):
        for h in range(3):
            head = 3 * g + h
            obuf[:, head * HD:(head + 1) * HD] = acc[g][h * T:(h + 1) * T].astype(BF16)

    phase('oproj')
    wait(ld_wo)
    hop1, hop2, hop3, hop4, hop5 = [], [], [], [], []
    def out_chunk(c):
        return [dot(obuf[...], cols(wo, slice(None), i * half + OUT_LO[c], OUT_W[c])) for i in range(2)]

    for group in OUT_GROUPS:
        for c in group:
            for i, p in enumerate(out_chunk(c)):
                part[i, :, span(c)] = p.astype(BF16)
        for c in group:
            hop1.append(remote(part.at[1 - core, :, span(c)], rx1.at[:, span(c)], r1.at[c], partner))
            hop1[c].start()
    phase('hop1')
    for c in range(NCH):
        hop1[c].wait_recv()
        cs[:, span(c)] = (part[core, :, span(c)].astype(F32) + rx1[:, span(c)].astype(F32)).astype(BF16)
        hop2.append(remote(cs.at[:, span(c)], rx2.at[:, span(c)], r2.at[c], across))
        hop2[c].start()

    phase('kvout')
    prow = lax.broadcasted_iota(jnp.int32, (2 * T, HD), 0)
    pcol = lax.broadcasted_iota(jnp.int32, (2 * T, HD), 1)
    for src, dst in ((kch, kout), (vch, vout)):
        mix = sum(dot(jnp.where(prow == 2 * pcol + g, 1.0, 0.0).astype(BF16), src[g]) for g in range(2))
        dst[...] = mix.astype(BF16)
    store_k = pltpu.make_async_copy(kout, kn_hbm.at[:2 * T], st_sem.at[0])
    store_v = pltpu.make_async_copy(vout, vn_hbm.at[:2 * T], st_sem.at[0])
    store_k.start()
    store_v.start()

    phase('hop2')
    for cp in x_sends:
        cp.wait_recv()
    gain2 = g2[...].astype(F32)
    g_top = jnp.maximum(jnp.max(jnp.max(jnp.abs(gain2), axis=1, keepdims=True), axis=0, keepdims=True), 1e-30)
    gain2 = gain2 / g_top
    wait(ld_gu)
    squares = []

    def gate_up(c):
        hop3[c].wait_recv()
        phase(f'gateup{c}')
        lo, w = OUT_LO[c], OUT_W[c]
        lhs = []
        for i in range(2):
            h32 = hbuf[i, :, span(c)].astype(F32)
            lhs.append((h32 * wide(gain2, i * half + lo, w)).astype(BF16))
            for j in range(w // 128):
                piece = h32[:, j * 128:(j + 1) * 128]
                squares.append(piece * piece if not squares else squares.pop() + piece * piece)
        lhs = jnp.concatenate([jnp.concatenate(lhs, axis=1), jnp.zeros((T, 2 * w), BF16)], axis=0)
        for k, ref in enumerate((wg, wu)):
            for n in range(0, F, 512):
                rhs = jnp.concatenate([cols(ref, slice(i * half + lo, i * half + lo + w), n, 512) for i in range(2)], axis=0)
                p = dot_padded(lhs, rhs)
                gacc[k, :, n:n + 512] = p if c == 0 else gacc[k, :, n:n + 512] + p

    for c in range(NCH):
        phase(f'hop2_{c}')
        hop2[c].wait_recv()
        total = cs[:, span(c)].astype(F32) + rx2[:, span(c)].astype(F32)
        hbuf[core, :, span(c)] = (xh[:, span(c)].astype(F32) + total).astype(BF16)
        hop3.append(remote(hbuf.at[core, :, span(c)], hbuf.at[core, :, span(c)], r3.at[c], partner))
        hop3[c].start()
        if c >= GLAG:
            gate_up(c - GLAG)
    for c in range(NCH - GLAG, NCH):
        phase(f'hop3_{c}')
        gate_up(c)
    phase('act')
    inv2 = lax.rsqrt(jnp.sum(squares[0], axis=-1, keepdims=True) / D + NORM_EPS)
    inv2 = inv2 * g_top
    gate = jnp.where(inv2 > 0, gacc[0] * inv2, 0.0)
    up = jnp.where(inv2 > 0, gacc[1] * inv2, 0.0)
    ubuf[:T] = (gate * jax.nn.sigmoid(gate) * up).astype(BF16)

    phase('down')
    wait(ld_wd)
    mine = rows_of(chip)
    theirs = rows_of(1 - chip)

    n_down = len(DOWN) - 1

    def chip_sum(c):
        hop4[c].wait_recv()
        at = slice(DOWN[c], DOWN[c + 1])
        cs2[:, at] = (part2[core, theirs, at].astype(F32) + rx4[theirs, at].astype(F32)).astype(BF16)
        hop5.append(remote(cs2.at[:, at], rx5.at[:, at], r5.at[c], across))
        hop5[c].start()

    for c in range(n_down):
        lo, hi = DOWN[c], DOWN[c + 1]
        p = dot_padded(ubuf[...], wd_cols(lo, hi - lo)).astype(BF16)
        for o in range(4):
            part2[o % 2, (o // 2) * tb:(o // 2 + 1) * tb, lo:hi] = p[o * tb:(o + 1) * tb]
        hop4.append(remote(part2.at[1 - core, :, lo:hi], rx4.at[:, lo:hi], r1.at[c], partner))
        hop4[c].start()
        if c >= LAG:
            chip_sum(c - LAG)
    phase('hop4')
    for c in range(n_down - LAG, n_down):
        chip_sum(c)
    phase('hop5')
    for c in range(n_down):
        hop5[c].wait_recv()
        for lo in range(DOWN[c], DOWN[c + 1], SLAB):
            at = slice(lo, lo + SLAB)
            h_own = hbuf[lo // half, own, lo % half:lo % half + SLAB].astype(F32)
            local = part2[core, mine, at].astype(F32) + rx4[mine, at].astype(F32) + rx5[:, at].astype(F32)
            xout[:, at] = (h_own + local).astype(BF16)
    store_x = pltpu.make_async_copy(xout, xo_hbm.at[:tb], st_sem.at[0])
    phase('fin')
    store_x.start()
    for cp in ag_a + [ag_p] + ag_f + x_sends + hop1 + hop2 + hop3 + hop4 + hop5:
        cp.wait_send()
    store_k.wait()
    store_v.wait()
    store_x.wait()
    phase.close()


def cache_kernel(start_ref, kc, vc, kch, vch, xin, kn, vn, xo, kbuf, vbuf, kcb, vcb, xb, in_sem, out_sem):
    nblk, per, _ = kc.shape
    rows = nblk * per
    small = [pltpu.make_async_copy(src, dst, in_sem.at[0]) for src, dst in ((kch.at[:kcb.shape[0]], kcb), (vch.at[:vcb.shape[0]], vcb), (xin.at[:xb.shape[0]], xb))]
    for cp in small:
        cp.start()
    first = lax.rem(2 * start_ref[0], rows)
    jrow = lax.broadcasted_iota(jnp.int32, (per, 128), 0)
    jcol = lax.broadcasted_iota(jnp.int32, (per, 128), 1)

    def touched(b):
        ahead = lax.rem(b * per - first + rows, rows)
        return (ahead < 128) | (ahead > rows - per)

    def writes(b, k_src, v_src):
        return [pltpu.make_async_copy(k_src.at[b], kn.at[b], out_sem.at[0]), pltpu.make_async_copy(v_src.at[b], vn.at[b], out_sem.at[0])]

    for b in range(nblk):
        @pl.when(jnp.logical_not(touched(b)))
        def _():
            for cp in writes(b, kc, vc):
                cp.start()

    for cp in small:
        cp.wait()
    x_write = pltpu.make_async_copy(xb, xo, out_sem.at[0])
    x_write.start()
    for b in range(nblk):
        @pl.when(touched(b))
        def _():
            rel = lax.rem(jrow + b * per - first + rows, rows)
            hot = jnp.where(rel == jcol, 1.0, 0.0).astype(BF16)
            inside = rel < 128
            kbuf[b] = jnp.where(inside, dot(hot, kcb[...]), kc[b].astype(F32)).astype(BF16)
            vbuf[b] = jnp.where(inside, dot(hot, vcb[...]), vc[b].astype(F32)).astype(BF16)
            for cp in writes(b, kbuf, vbuf):
                cp.start()

    x_write.wait()
    for b in range(nblk):
        for cp in writes(b, kbuf, vbuf):
            cp.wait()


def solution(mesh):
    row_spec = P('dp', 'tp', None)
    cache_spec = P('dp', None, 'tp', None)
    head_cols = P(None, 'tp', None)
    in_specs = (row_spec, P('dp'), cache_spec, cache_spec, P(), head_cols, head_cols, head_cols, P('tp', None, None), P(), P(None, 'tp'), P(None, 'tp'), P('tp', None))
    out_specs = (row_spec, cache_spec, cache_spec)

    def local_layer(x_in, start_pos, k_cache, v_cache, attn_gain, w_query, w_key, w_value, w_out, mlp_gain, w_gate, w_up, w_down):
        _, tb, D = x_in.shape
        T = 4 * tb
        window = k_cache.shape[1]
        F = w_gate.shape[1]
        qh = w_query.shape[1]
        invf = jnp.asarray(np.repeat(ROPE_BASE ** (-np.arange(0, HD, 2) / HD), 2).astype(np.float32)[None])
        blocks = window // 128
        kc = k_cache.reshape(blocks, 256, HD)
        vc = v_cache.reshape(blocks, 256, HD)
        wk = w_key.reshape(D // 128, 256, HD)
        wv = w_value.reshape(D // 128, 256, HD)
        any_spec = pl.BlockSpec(memory_space=pl.ANY)
        vmem = pltpu.VMEM
        dma = pltpu.SemaphoreType.DMA
        x_out, k_ch, v_ch = pl.pallas_call(
            layer_kernel,
            name='layer',
            out_shape=(jax.ShapeDtypeStruct((SPARE // D, D), BF16), jax.ShapeDtypeStruct((SPARE // HD, HD), BF16), jax.ShapeDtypeStruct((SPARE // HD, HD), BF16)),
            in_specs=[any_spec] * 14,
            out_specs=(any_spec,) * 3,
            scratch_shapes=[
                pltpu.SMEM((1,), jnp.int32), vmem((1, HD), F32),
                vmem((tb, D), BF16), vmem((T, D // 2), BF16), vmem((T, D), BF16), vmem((D // HD, HD), BF16), vmem((D // HD, HD), BF16),
                vmem((blocks, 256, HD), BF16), vmem((blocks, 256, HD), BF16),
                vmem((qh * D, HD), BF16), vmem((D // 128, 256, HD), BF16), vmem((D // 128, 256, HD), BF16),
                vmem((D // SLAB, qh * HD, SLAB), BF16), vmem((F // SLAB, D, SLAB), BF16), vmem((F // SLAB, D, SLAB), BF16), vmem((D // HD - qh * D // F, F, HD), BF16),
                vmem((5, T, 256), F32), vmem((8, window), jnp.int32),
                vmem((2, window // KB, 3 * T, KB), F32), vmem((2, 3 * T, HD), BF16), vmem((2, 128, HD), BF16), vmem((2, 128, HD), BF16),
                vmem((T, qh * HD), BF16),
                vmem((2, T, D // 2), BF16), vmem((T, D // 2), BF16), vmem((T, D // 2), BF16), vmem((T, D // 2), BF16),
                vmem((2, T, D // 2), BF16), vmem((2, T, F), F32), vmem((2 * T, F), BF16),
                vmem((2, 2 * tb, D), BF16), vmem((2 * tb, D), BF16), vmem((tb, D), BF16), vmem((tb, D), BF16),
                vmem((tb, D), BF16), vmem((2 * T, HD), BF16), vmem((2 * T, HD), BF16),
                dma((8,)), dma((1,)), dma((1,)), dma((1,))] + [dma((NAG,)), dma((3,))] + [dma((NCH,))] * 3 + [dma((len(DOWN) - 1,))],
            compiler_params=pltpu.CompilerParams(collective_id=0, has_side_effects=True, vmem_limit_bytes=LAYER_VMEM),
            cost_estimate=pl.CostEstimate(flops=2 * 64 * 25 * 10**6, bytes_accessed=80 * 10**6, transcendentals=3 * 10**6),
        )(start_pos, invf, x_in.reshape(tb, D), attn_gain.reshape(D // HD, HD), mlp_gain.reshape(D // HD, HD), kc, vc, w_query.transpose(1, 0, 2).reshape(qh * D, HD), wk, wv,
          w_out.reshape(qh * HD, D), w_gate, w_up, w_down)
        nblk = 16
        per = 2 * window // nblk
        k_new, v_new, x_fin = pl.pallas_call(
            cache_kernel,
            name='cache',
            out_shape=(jax.ShapeDtypeStruct((nblk, per, HD), BF16),) * 2 + (jax.ShapeDtypeStruct((tb, D), BF16),),
            in_specs=[pl.BlockSpec(memory_space=pltpu.SMEM)] + [pl.BlockSpec(memory_space=pltpu.VMEM)] * 2 + [pl.BlockSpec(memory_space=pltpu.HBM)] * 3,
            out_specs=(any_spec,) * 3,
            scratch_shapes=[vmem((nblk, per, HD), BF16)] * 2 + [vmem((2 * T, HD), BF16)] * 2 + [vmem((tb, D), BF16), dma((1,)), dma((1,))],
            compiler_params=pltpu.CompilerParams(vmem_limit_bytes=CACHE_VMEM),
        )(start_pos, k_cache.reshape(nblk, per, HD), v_cache.reshape(nblk, per, HD), k_ch, v_ch, x_out)
        return x_fin.reshape(x_in.shape), k_new.reshape(k_cache.shape), v_new.reshape(v_cache.shape)

    return jax.shard_map(local_layer, mesh=mesh, in_specs=in_specs, out_specs=out_specs, check_vma=False)
```

```python
import functools

import jax
import jax.numpy as jnp
import numpy as np
from jax import lax
from jax.experimental import pallas as pl
from jax.experimental.pallas import tpu as pltpu
from jax.sharding import PartitionSpec as P

ROPE_BASE = 10000.0
NORM_EPS = 1e-5
MESH = pl.DeviceIdType.MESH
BF16 = jnp.bfloat16
F32 = jnp.float32
HD = 128
OUT_W = (256, 256, 256, 256, 256, 256)
OUT_LO = tuple(sum(OUT_W[:i]) for i in range(len(OUT_W)))
NCH = len(OUT_W)
OUT_GROUPS = ((0,), (1, 2), (3, 4, 5))
DOWN = (0, 1024, 2048, 2560, 3072)
NAG = 4
LAG = 2
GLAG = 2
PADQ = True
PVN = 4
KB = 512
SLAB = 256
LAYER_VMEM = 62600000
CACHE_VMEM = 24 * 10**6
SPARE = 3 * 2**23


def dot(a, b):
    return jnp.dot(a, b, preferred_element_type=F32)


def dot_padded(a, b):
    p = dot(a, b)
    m = a.shape[0] // 2
    return p[:m] + p[m:]


def dot_t(a, b):
    return lax.dot_general(a, b, (((1,), (1,)), ((), ())), preferred_element_type=F32)


class Phases:
    def __init__(self):
        self.scope = None

    def __call__(self, name):
        self.close()
        self.scope = jax.named_scope(name)
        self.scope.__enter__()

    def close(self):
        if self.scope is not None:
            self.scope.__exit__(None, None, None)
        self.scope = None


def layer_kernel(start_hbm, invf_hbm, x_hbm, g1_hbm, g2_hbm, kc_hbm, vc_hbm, wq_hbm, wk_hbm, wv_hbm, wo_hbm, wg_hbm, wu_hbm, wd_hbm,
                 xo_hbm, kn_hbm, vn_hbm,
                 start_s, invf, xown, xh, nbuf, g1, g2, kbuf, vbuf, wq, wk, wv, wo, wg, wu, wd,
                 qacc, offb, sbuf, qbuf, kch, vch, obuf, part, rx1, cs, rx2, hbuf, gacc, ubuf, part2, rx4, cs2, rx5, xout, kout, vout,
                 ld_sem, st_sem, out_sem, agp_r, aga_r, xs_r, r1, r2, r3, r5):
    phase = Phases()
    phase('entry')
    T, D = nbuf.shape
    half = D // 2
    AW = D // NAG
    tb = T // 4
    window = kbuf.shape[0] * 128
    F = wg.shape[0] * SLAB
    me = lax.axis_index('tp')
    core = lax.rem(me, 2)
    chip = lax.div(me, 2)
    partner = chip * 2 + (1 - core)
    across = (1 - chip) * 2 + core
    diag = (1 - chip) * 2 + (1 - core)

    def load(i, src, dst):
        return pltpu.make_async_copy(src, dst, ld_sem.at[i])

    def slabs(i, src, dst):
        return [load(i, src.at[:, j * SLAB:(j + 1) * SLAB], dst.at[j]) for j in range(dst.shape[0])]

    def cols(ref, rows, lo, n):
        parts = [ref[j * HD // SLAB, rows, j * HD % SLAB:j * HD % SLAB + HD] for j in range(lo // HD, (lo + n) // HD)]
        return parts[0] if len(parts) == 1 else jnp.concatenate(parts, axis=1)

    def span(c):
        return slice(OUT_LO[c], OUT_LO[c] + OUT_W[c])

    def rows_of(owner):
        return pl.ds(pl.multiple_of(owner * tb, tb), tb)

    def half_of(which):
        return pl.ds(pl.multiple_of(which * half, 128), half)

    def remote(src, dst, recv, dev):
        return pltpu.make_async_remote_copy(src_ref=src, dst_ref=dst, send_sem=out_sem.at[0], recv_sem=recv, device_id={'tp': dev}, device_id_type=MESH)

    def wide(gain, lo, n):
        return jnp.concatenate([gain[i:i + 1] for i in range(lo // HD, (lo + n) // HD)], axis=1)

    barrier = pltpu.get_barrier_semaphore()
    for other in (across, diag, partner):
        pl.semaphore_signal(barrier, inc=1, device_id={'tp': other}, device_id_type=MESH)

    own = rows_of(me)
    ld_x = [load(0, x_hbm, xown), load(0, g1_hbm, g1)]
    ld_small = [load(1, g2_hbm, g2), load(1, start_hbm, start_s), load(1, invf_hbm, invf), load(1, x_hbm.at[:, half_of(core)], xh.at[own])]
    ld_cache = [load(2, kc_hbm, kbuf), load(2, vc_hbm, vbuf)]
    ld_wkv = [load(3, wk_hbm, wk), load(3, wv_hbm, wv)]
    ld_wq = [load(4, wq_hbm, wq)]
    ld_wo = slabs(5, wo_hbm, wo)
    ld_gu = slabs(6, wg_hbm, wg) + slabs(6, wu_hbm, wu)
    n_main = wd.shape[0]
    wd_slabs = [wd.at[j] if j < n_main else wq.at[pl.ds((j - n_main) * F, F)] for j in range(D // HD)]
    ld_wd = [load(7, wd_hbm.at[:, j * HD:(j + 1) * HD], wd_slabs[j]) for j in range(D // HD)]

    def wd_cols(lo, n):
        return jnp.concatenate([wd_slabs[j][...] for j in range(lo // HD, (lo + n) // HD)], axis=1)

    def wait(group):
        for item in group:
            item.wait()

    for item in ld_x + ld_small + ld_cache + ld_wkv + ld_wq + ld_wo + ld_gu + ld_wd[:n_main]:
        item.start()

    wait(ld_x)
    x32 = xown[...].astype(F32)
    inv = lax.rsqrt(jnp.mean(x32 * x32, axis=-1, keepdims=True) + NORM_EPS)
    nbuf[own] = (x32 * inv * wide(g1[...].astype(F32), 0, D)).astype(BF16)
    pl.semaphore_wait(barrier, 3)
    ag_a = []
    for c in range(NAG):
        piece = nbuf.at[own, pl.ds(c * AW, AW)]
        ag_a.append(remote(piece, piece, aga_r.at[c], across))
        ag_a[c].start()
    ag_p = remote(nbuf.at[own], nbuf.at[own], agp_r.at[0], partner)
    ag_p.start()

    phase('trig')
    wait(ld_small)
    start = start_s[0]
    lane = lax.broadcasted_iota(jnp.int32, (T, HD), 1)
    tok = lax.broadcasted_iota(jnp.int32, (T, HD), 0)
    angles = (start + tok).astype(F32) * invf[...]
    cos_t = jnp.cos(angles)
    even = lax.rem(lane, 2) == 0
    sin_t = jnp.sin(angles)
    sin_t = jnp.where(even, -sin_t, sin_t)
    slot = lax.broadcasted_iota(jnp.int32, (8, window), 1)
    off = lax.rem(slot - start + 4 * window, window)
    offb[...] = jnp.where(start - window + off >= 0, off, -1)

    def rope(h):
        swapped = jnp.where(even, pltpu.roll(h, HD - 1, 1), pltpu.roll(h, 1, 1))
        return h * cos_t + swapped * sin_t

    row = lax.broadcasted_iota(jnp.int32, (256, 256), 0)
    col = lax.broadcasted_iota(jnp.int32, (256, 256), 1)
    pick = jnp.where(col == 2 * lax.rem(row, 128) + lax.div(row, 128), 1.0, 0.0).astype(BF16)

    def split(a_ref, b_ref, lo, hi):
        def body(b, carry):
            both = jnp.concatenate([a_ref[b], b_ref[b]], axis=1)
            sep = dot(pick, both).astype(BF16)
            a_ref[b] = sep[:, :128]
            b_ref[b] = sep[:, 128:]
            return carry
        lax.fori_loop(lo, hi, body, 0, unroll=12 if (hi - lo) % 12 == 0 else 16)

    phase('wait_cache')
    wait(ld_cache)
    phase('split_cache')
    split(kbuf, vbuf, 0, kbuf.shape[0])
    phase('wait_wkv')
    wait(ld_wkv)
    ag_f = []

    def relay(c):
        ag_a[c].wait_recv()
        piece = nbuf.at[rows_of(across), pl.ds(c * AW, AW)]
        ag_f.append(remote(piece, piece, r3.at[c], partner))
        ag_f[c].start()

    phase('split_wkv')
    split(wk, wv, 0, wk.shape[0])
    for c in range(NAG):
        phase(f'wait_across{c}')
        relay(c)

    x_sends = [remote(xown.at[:, half_of(core)], xh.at[own], xs_r.at[0], across),
               remote(xown.at[:, half_of(1 - core)], xh.at[own], xs_r.at[1], diag),
               remote(xown.at[:, half_of(1 - core)], xh.at[own], xs_r.at[2], partner)]
    for cp in x_sends:
        cp.start()

    QW = AW
    per_q = QW // 128

    def split_rows(ref, g, c):
        return ref[c * per_q:(c + 1) * per_q, g * 128:(g + 1) * 128, :].reshape(QW, HD)

    ag_p.wait_recv()
    wait(ld_wq)
    ubuf[T:] = jnp.zeros((T, F), BF16)
    kch[...] = jnp.zeros_like(kch)
    vch[...] = jnp.zeros_like(vch)
    for c in range(NAG):
        phase(f'wait_fwd{c}')
        ag_f[c].wait_recv()
        phase(f'qkv{c}')
        rows = nbuf[:, c * QW:(c + 1) * QW]
        w = [wq[h * D + c * QW:h * D + (c + 1) * QW] for h in range(6)]
        w += [split_rows(ref, g, c) for ref in (wk, wv) for g in range(2)]
        p = dot_padded(jnp.concatenate([rows, jnp.zeros_like(rows)], axis=0), jnp.concatenate(w, axis=1)) if PADQ else dot(rows, jnp.concatenate(w, axis=1))
        for o in range(5):
            q = p[:, o * 256:(o + 1) * 256]
            qacc[o] = q if c == 0 else qacc[o] + q
    phase('rope')

    for g in range(2):
        kch[g, :T] = rope(qacc[3, :, g * HD:(g + 1) * HD]).astype(BF16)
        vch[g, :T] = qacc[4, :, g * HD:(g + 1) * HD].astype(BF16)
    for head in range(6):
        qbuf[head // 3, (head % 3) * T:(head % 3 + 1) * T] = rope(qacc[head // 2, :, (head % 2) * HD:(head % 2 + 1) * HD]).astype(BF16)

    phase('attn')
    coef = HD ** -0.5 * float(np.log2(np.e))
    nblk = window // KB
    nb = KB // 128
    q_tok = lax.broadcasted_iota(jnp.int32, (T, HD), 0)
    q_tok3 = q_tok.reshape(T // 8, 8, HD)
    k_idx = lax.broadcasted_iota(jnp.int32, (T, HD), 1)

    def blocks(ref, g, i):
        return ref[i * nb:(i + 1) * nb, g * 128:(g + 1) * 128, :].reshape(KB, HD)

    top, mass, s_c = [[None] * 3, [None] * 3], [[None] * 3, [None] * 3], [[None] * 3, [None] * 3]
    peak, e_c, scale, acc = [[None] * 3, [None] * 3], [[None] * 3, [None] * 3], [[None] * 3, [None] * 3], [None, None]

    def score_chunk(g):
        s = dot_t(qbuf[g], kch[g])
        for h in range(3):
            s_c[g][h] = jnp.where(k_idx <= q_tok, s[h * T:(h + 1) * T], -jnp.inf)
            top[g][h] = s_c[g][h]

    def score(g, i):
        s = dot_t(qbuf[g], blocks(kbuf, g, i))
        for j in range(nb):
            o = offb[:, i * KB + j * 128:i * KB + (j + 1) * 128][None]
            keep = o > q_tok3
            for h in range(3):
                piece = s[h * T:(h + 1) * T, j * 128:(j + 1) * 128].reshape(T // 8, 8, HD)
                piece = jnp.where(keep, piece, -jnp.inf).reshape(T, HD)
                sbuf[g, i, h * T:(h + 1) * T, j * 128:(j + 1) * 128] = piece
                top[g][h] = jnp.maximum(top[g][h], piece)

    def expo_chunk(g):
        for h in range(3):
            peak[g][h] = jnp.max(top[g][h], axis=1, keepdims=True)
            e_c[g][h] = jnp.exp2((s_c[g][h] - peak[g][h]) * coef)
            mass[g][h] = e_c[g][h]

    def expo(g, h, i):
        e = jnp.exp2((sbuf[g, i, h * T:(h + 1) * T] - peak[g][h]) * coef)
        sbuf[g, i, h * T:(h + 1) * T] = e
        for j in range(nb):
            mass[g][h] = mass[g][h] + e[:, j * 128:(j + 1) * 128]

    parts = [[], []]

    def weigh_chunk(g):
        for h in range(3):
            scale[g][h] = 1.0 / jnp.sum(mass[g][h], axis=1, keepdims=True)
        parts[g].append(jnp.concatenate([(e_c[g][h] * scale[g][h]).astype(BF16) for h in range(3)], axis=0))

    def weigh(g, i):
        parts[g].append(jnp.concatenate([(sbuf[g, i, h * T:(h + 1) * T] * scale[g][h]).astype(BF16) for h in range(3)], axis=0))
        if i == nblk - 1:
            acc[g] = dot(parts[g][0], vch[g])
            n = PVN
            for k in range(0, nblk, n):
                p = jnp.concatenate(parts[g][1 + k:1 + k + n], axis=1)
                acc[g] = acc[g] + dot(p, jnp.concatenate([blocks(vbuf, g, j) for j in range(k, k + n)], axis=0))

    order = [(h, i) for h in range(3) for i in range(nblk)]
    score_chunk(0)
    for i in range(nblk):
        score(0, i)
    score_chunk(1)
    expo_chunk(0)
    for i in range(nblk):
        score(1, i)
        for h, k in order[3 * i:3 * i + 3]:
            expo(0, h, k)
    expo_chunk(1)
    weigh_chunk(0)
    for i in range(nblk):
        weigh(0, i)
        for h, k in order[3 * i:3 * i + 3]:
            expo(1, h, k)
    weigh_chunk(1)
    for i in range(nblk):
        weigh(1, i)
    for g in range(2):
        for h in range(3):
            head = 3 * g + h
            obuf[:, head * HD:(head + 1) * HD] = acc[g][h * T:(h + 1) * T].astype(BF16)

    phase('oproj')
    wait(ld_wo)
    hop1, hop2, hop3, hop4, hop5 = [], [], [], [], []
    def out_chunk(c):
        return [dot(obuf[...], cols(wo, slice(None), i * half + OUT_LO[c], OUT_W[c])) for i in range(2)]

    for group in OUT_GROUPS:
        for c in group:
            for i, p in enumerate(out_chunk(c)):
                part[i, :, span(c)] = p.astype(BF16)
        for c in group:
            hop1.append(remote(part.at[1 - core, :, span(c)], rx1.at[:, span(c)], r1.at[c], partner))
            hop1[c].start()
    phase('hop1')
    for c in range(NCH):
        hop1[c].wait_recv()
        cs[:, span(c)] = (part[core, :, span(c)].astype(F32) + rx1[:, span(c)].astype(F32)).astype(BF16)
        hop2.append(remote(cs.at[:, span(c)], rx2.at[:, span(c)], r2.at[c], across))
        hop2[c].start()

    phase('kvout')
    for item in ld_wd[n_main:]:
        item.start()
    prow = lax.broadcasted_iota(jnp.int32, (2 * T, HD), 0)
    pcol = lax.broadcasted_iota(jnp.int32, (2 * T, HD), 1)
    for src, dst in ((kch, kout), (vch, vout)):
        mix = sum(dot(jnp.where(prow == 2 * pcol + g, 1.0, 0.0).astype(BF16), src[g]) for g in range(2))
        dst[...] = mix.astype(BF16)
    store_k = pltpu.make_async_copy(kout, kn_hbm.at[:2 * T], st_sem.at[0])
    store_v = pltpu.make_async_copy(vout, vn_hbm.at[:2 * T], st_sem.at[0])
    store_k.start()
    store_v.start()

    phase('hop2')
    for cp in x_sends:
        cp.wait_recv()
    gain2 = g2[...].astype(F32)
    g_top = jnp.maximum(jnp.max(jnp.max(jnp.abs(gain2), axis=1, keepdims=True), axis=0, keepdims=True), 1e-30)
    gain2 = gain2 / g_top
    wait(ld_gu)
    squares = []

    def gate_up(c):
        hop3[c].wait_recv()
        phase(f'gateup{c}')
        lo, w = OUT_LO[c], OUT_W[c]
        lhs = []
        for i in range(2):
            h32 = hbuf[i, :, span(c)].astype(F32)
            lhs.append((h32 * wide(gain2, i * half + lo, w)).astype(BF16))
            for j in range(w // 128):
                piece = h32[:, j * 128:(j + 1) * 128]
                squares.append(piece * piece if not squares else squares.pop() + piece * piece)
        lhs = jnp.concatenate([jnp.concatenate(lhs, axis=1), jnp.zeros((T, 2 * w), BF16)], axis=0)
        last = c == NCH - 1
        if last:
            inv2 = lax.rsqrt(jnp.sum(squares[0], axis=-1, keepdims=True) / D + NORM_EPS)
            inv2 = inv2 * g_top
        for n in range(0, F, 512):
            both = []
            for k, ref in enumerate((wg, wu)):
                rhs = jnp.concatenate([cols(ref, slice(i * half + lo, i * half + lo + w), n, 512) for i in range(2)], axis=0)
                p = dot_padded(lhs, rhs)
                p = p if c == 0 else gacc[k, :, n:n + 512] + p
                if last:
                    both.append(jnp.where(inv2 > 0, p * inv2, 0.0))
                else:
                    gacc[k, :, n:n + 512] = p
            if last:
                ubuf[:T, n:n + 512] = (both[0] * jax.nn.sigmoid(both[0]) * both[1]).astype(BF16)

    for c in range(NCH):
        phase(f'hop2_{c}')
        hop2[c].wait_recv()
        total = cs[:, span(c)].astype(F32) + rx2[:, span(c)].astype(F32)
        hbuf[core, :, span(c)] = (xh[:, span(c)].astype(F32) + total).astype(BF16)
        hop3.append(remote(hbuf.at[core, :, span(c)], hbuf.at[core, :, span(c)], r3.at[c], partner))
        hop3[c].start()
        if c >= GLAG:
            gate_up(c - GLAG)
    for c in range(NCH - GLAG, NCH):
        phase(f'hop3_{c}')
        gate_up(c)
    phase('down')
    wait(ld_wd)
    mine = rows_of(chip)
    theirs = rows_of(1 - chip)

    n_down = len(DOWN) - 1

    def chip_sum(c):
        hop4[c].wait_recv()
        at = slice(DOWN[c], DOWN[c + 1])
        cs2[:, at] = (part2[core, theirs, at].astype(F32) + rx4[theirs, at].astype(F32)).astype(BF16)
        hop5.append(remote(cs2.at[:, at], rx5.at[:, at], r5.at[c], across))
        hop5[c].start()

    for c in range(n_down):
        lo, hi = DOWN[c], DOWN[c + 1]
        p = dot_padded(ubuf[...], wd_cols(lo, hi - lo)).astype(BF16)
        for o in range(4):
            part2[o % 2, (o // 2) * tb:(o // 2 + 1) * tb, lo:hi] = p[o * tb:(o + 1) * tb]
        hop4.append(remote(part2.at[1 - core, :, lo:hi], rx4.at[:, lo:hi], r1.at[c], partner))
        hop4[c].start()
        if c >= LAG:
            chip_sum(c - LAG)
    phase('hop4')
    for c in range(n_down - LAG, n_down):
        chip_sum(c)
    phase('hop5')
    for c in range(n_down):
        hop5[c].wait_recv()
        for lo in range(DOWN[c], DOWN[c + 1], SLAB):
            at = slice(lo, lo + SLAB)
            h_own = hbuf[lo // half, own, lo % half:lo % half + SLAB].astype(F32)
            local = part2[core, mine, at].astype(F32) + rx4[mine, at].astype(F32) + rx5[:, at].astype(F32)
            xout[:, at] = (h_own + local).astype(BF16)
    store_x = pltpu.make_async_copy(xout, xo_hbm.at[:tb], st_sem.at[0])
    phase('fin')
    store_x.start()
    for cp in ag_a + [ag_p] + ag_f + x_sends + hop1 + hop2 + hop3 + hop4 + hop5:
        cp.wait_send()
    store_k.wait()
    store_v.wait()
    store_x.wait()
    phase.close()


def cache_kernel(start_ref, kc, vc, kch, vch, xin, kn, vn, xo, kbuf, vbuf, kcb, vcb, xb, in_sem, out_sem):
    nblk, per, _ = kc.shape
    rows = nblk * per
    small = [pltpu.make_async_copy(src, dst, in_sem.at[0]) for src, dst in ((kch.at[:kcb.shape[0]], kcb), (vch.at[:vcb.shape[0]], vcb), (xin.at[:xb.shape[0]], xb))]
    for cp in small:
        cp.start()
    first = lax.rem(2 * start_ref[0], rows)
    jrow = lax.broadcasted_iota(jnp.int32, (per, 128), 0)
    jcol = lax.broadcasted_iota(jnp.int32, (per, 128), 1)

    def touched(b):
        ahead = lax.rem(b * per - first + rows, rows)
        return (ahead < 128) | (ahead > rows - per)

    def writes(b, k_src, v_src):
        return [pltpu.make_async_copy(k_src.at[b], kn.at[b], out_sem.at[0]), pltpu.make_async_copy(v_src.at[b], vn.at[b], out_sem.at[0])]

    for b in range(nblk):
        @pl.when(jnp.logical_not(touched(b)))
        def _():
            for cp in writes(b, kc, vc):
                cp.start()

    for cp in small:
        cp.wait()
    x_write = pltpu.make_async_copy(xb, xo, out_sem.at[0])
    x_write.start()
    for b in range(nblk):
        @pl.when(touched(b))
        def _():
            rel = lax.rem(jrow + b * per - first + rows, rows)
            hot = jnp.where(rel == jcol, 1.0, 0.0).astype(BF16)
            inside = rel < 128
            kbuf[b] = jnp.where(inside, dot(hot, kcb[...]), kc[b].astype(F32)).astype(BF16)
            vbuf[b] = jnp.where(inside, dot(hot, vcb[...]), vc[b].astype(F32)).astype(BF16)
            for cp in writes(b, kbuf, vbuf):
                cp.start()

    x_write.wait()
    for b in range(nblk):
        for cp in writes(b, kbuf, vbuf):
            cp.wait()


def solution(mesh):
    row_spec = P('dp', 'tp', None)
    cache_spec = P('dp', None, 'tp', None)
    head_cols = P(None, 'tp', None)
    in_specs = (row_spec, P('dp'), cache_spec, cache_spec, P(), head_cols, head_cols, head_cols, P('tp', None, None), P(), P(None, 'tp'), P(None, 'tp'), P('tp', None))
    out_specs = (row_spec, cache_spec, cache_spec)

    def local_layer(x_in, start_pos, k_cache, v_cache, attn_gain, w_query, w_key, w_value, w_out, mlp_gain, w_gate, w_up, w_down):
        _, tb, D = x_in.shape
        T = 4 * tb
        window = k_cache.shape[1]
        F = w_gate.shape[1]
        qh = w_query.shape[1]
        invf = jnp.asarray(np.repeat(ROPE_BASE ** (-np.arange(0, HD, 2) / HD), 2).astype(np.float32)[None])
        blocks = window // 128
        kc = k_cache.reshape(blocks, 256, HD)
        vc = v_cache.reshape(blocks, 256, HD)
        wk = w_key.reshape(D // 128, 256, HD)
        wv = w_value.reshape(D // 128, 256, HD)
        any_spec = pl.BlockSpec(memory_space=pl.ANY)
        vmem = pltpu.VMEM
        dma = pltpu.SemaphoreType.DMA
        x_out, k_ch, v_ch = pl.pallas_call(
            layer_kernel,
            name='layer',
            out_shape=(jax.ShapeDtypeStruct((SPARE // D, D), BF16), jax.ShapeDtypeStruct((SPARE // HD, HD), BF16), jax.ShapeDtypeStruct((SPARE // HD, HD), BF16)),
            in_specs=[any_spec] * 14,
            out_specs=(any_spec,) * 3,
            scratch_shapes=[
                pltpu.SMEM((1,), jnp.int32), vmem((1, HD), F32),
                vmem((tb, D), BF16), vmem((T, D // 2), BF16), vmem((T, D), BF16), vmem((D // HD, HD), BF16), vmem((D // HD, HD), BF16),
                vmem((blocks, 256, HD), BF16), vmem((blocks, 256, HD), BF16),
                vmem((qh * D, HD), BF16), vmem((D // 128, 256, HD), BF16), vmem((D // 128, 256, HD), BF16),
                vmem((D // SLAB, qh * HD, SLAB), BF16), vmem((F // SLAB, D, SLAB), BF16), vmem((F // SLAB, D, SLAB), BF16), vmem((D // HD - qh * D // F, F, HD), BF16),
                vmem((5, T, 256), F32), vmem((8, window), jnp.int32),
                vmem((2, window // KB, 3 * T, KB), F32), vmem((2, 3 * T, HD), BF16), vmem((2, 128, HD), BF16), vmem((2, 128, HD), BF16),
                vmem((T, qh * HD), BF16),
                vmem((2, T, D // 2), BF16), vmem((T, D // 2), BF16), vmem((T, D // 2), BF16), vmem((T, D // 2), BF16),
                vmem((2, T, D // 2), BF16), vmem((2, T, F), F32), vmem((2 * T, F), BF16),
                vmem((2, 2 * tb, D), BF16), vmem((2 * tb, D), BF16), vmem((tb, D), BF16), vmem((tb, D), BF16),
                vmem((tb, D), BF16), vmem((2 * T, HD), BF16), vmem((2 * T, HD), BF16),
                dma((8,)), dma((1,)), dma((1,)), dma((1,))] + [dma((NAG,)), dma((3,))] + [dma((NCH,))] * 3 + [dma((len(DOWN) - 1,))],
            compiler_params=pltpu.CompilerParams(collective_id=0, has_side_effects=True, vmem_limit_bytes=LAYER_VMEM),
            cost_estimate=pl.CostEstimate(flops=2 * 64 * 25 * 10**6, bytes_accessed=80 * 10**6, transcendentals=3 * 10**6),
        )(start_pos, invf, x_in.reshape(tb, D), attn_gain.reshape(D // HD, HD), mlp_gain.reshape(D // HD, HD), kc, vc, w_query.transpose(1, 0, 2).reshape(qh * D, HD), wk, wv,
          w_out.reshape(qh * HD, D), w_gate, w_up, w_down)
        nblk = 16
        per = 2 * window // nblk
        k_new, v_new, x_fin = pl.pallas_call(
            cache_kernel,
            name='cache',
            out_shape=(jax.ShapeDtypeStruct((nblk, per, HD), BF16),) * 2 + (jax.ShapeDtypeStruct((tb, D), BF16),),
            in_specs=[pl.BlockSpec(memory_space=pltpu.SMEM)] + [pl.BlockSpec(memory_space=pltpu.VMEM)] * 2 + [pl.BlockSpec(memory_space=pltpu.HBM)] * 3,
            out_specs=(any_spec,) * 3,
            scratch_shapes=[vmem((nblk, per, HD), BF16)] * 2 + [vmem((2 * T, HD), BF16)] * 2 + [vmem((tb, D), BF16), dma((1,)), dma((1,))],
            compiler_params=pltpu.CompilerParams(vmem_limit_bytes=CACHE_VMEM),
        )(start_pos, k_cache.reshape(nblk, per, HD), v_cache.reshape(nblk, per, HD), k_ch, v_ch, x_out)
        return x_fin.reshape(x_in.shape), k_new.reshape(k_cache.shape), v_new.reshape(v_cache.shape)

    return jax.shard_map(local_layer, mesh=mesh, in_specs=in_specs, out_specs=out_specs, check_vma=False)
```
